128 devices in a mesh: dom: 8 (over z, core), feat: 16 (over x, y).
Axes of the slice: x: 4, y: 4, z: 4, core: 2. Of those that a mesh axis runs over, the one named last changes fastest.
Arguments:
- node_feats: bfloat16 [8192, 512], P('dom', 'feat'), may hold values from -6 to 6
- rel_weight: bfloat16 [4, 512, 512], replicated, may hold values from -0.25 to 0.25
- self_weight: bfloat16 [512, 512], replicated, may hold values from -0.25 to 0.25
- bias: float32 [512], replicated, may hold values from -3 to 3
- out_degree: int32 [4, 8192], P(None, 'dom'), may hold values from 0 to 63
- adjacency: int32 [8, 16, 64, 256, 256], P('dom', 'feat'), may hold values 0 or 1
- tile_index: int32 [8, 16, 64, 3], P('dom', 'feat'), may hold values from 0 to 31, as said below
- tile_count: int32 [8, 16], P('dom', 'feat'), may hold values from 1 to 64, as said below
Outputs:
- embedding: bfloat16 [8192, 512], P('dom', 'feat')
The draws below stay inside these ranges and needn't reach their ends.
Inputs may be any that keep to these rules, and one draw needn't show every extreme that they name: `tile_index`: the three entries of a slot are a relation below 4, a destination block below 32 and a source block of the device's own group below 4; entries of slots beyond a device's count are arbitrary within the range. `tile_count`: some device holds exactly 64 live slots.
All inputs are finite; a program needn't handle non-finite values. No bound on the sum of `adjacency` on one device may be relied on, other than what follows from the above.
Results may differ from the reference program's by a relative error of at most 0.0049.
Values may be sent and summed in bfloat16 or wider, within the bound.
A program may use at most 128 MiB of HBM per device.

```python
import jax
import jax.numpy as jnp
from jax import lax

H = 512
R = 4
TILE_SIZE = 256
BG = 4
TILE_DEV = 64
NODES = 8192
N_DOM = 8
N_FEAT = 16


def draw_tile_index(key, part):
    first, second, third = jax.random.split(jax.random.fold_in(key, 11), 3)
    shape = (N_DOM, N_FEAT, TILE_DEV)
    relation = jax.random.randint(first, shape, 0, R)
    target = jax.random.randint(second, shape, 0, N_DOM * BG)
    source = jax.random.randint(third, shape, 0, BG)
    return jnp.stack([relation, target, source], axis=-1).astype(jnp.int32)


def draw_tile_count(key, part):
    first, second = jax.random.split(jax.random.fold_in(key, 23), 2)
    counts = jax.random.randint(first, (N_DOM * N_FEAT,), 1, TILE_DEV + 1)
    position = jax.random.randint(second, (), 0, N_DOM * N_FEAT)
    positions = jnp.arange(N_DOM * N_FEAT)
    counts = jnp.where(positions == position, TILE_DEV, counts)
    return counts.reshape(N_DOM, N_FEAT).astype(jnp.int32)


def touch_ends(result, stream_key, low, largest):
    spot = [jax.random.randint(jax.random.fold_in(stream_key, axis), (), 0, length) for axis, length in enumerate(result.shape)]
    longest = result.shape.index(max(result.shape))
    next_to = spot[:longest] + [(spot[longest] + 1) % result.shape[longest]] + spot[longest + 1:]
    return result.at[tuple(spot)].set(low).at[tuple(next_to)].set(largest)


def block_levels(stream_key, shape, cuts, low, largest):
    factor_of, own = 1.0, jax.random.fold_in(stream_key, 6)
    for axis_at, blocks in cuts:
        heights = jnp.exp(jax.random.uniform(jax.random.fold_in(own, axis_at), (blocks,), jnp.float32, low / len(cuts), largest / len(cuts)))
        factor_of = factor_of * jnp.repeat(heights, shape[axis_at] // blocks).reshape([-1 if axis == axis_at else 1 for axis in range(len(shape))])
    return factor_of


def noise(stream_key, extent, spread, reach, pieces=(), kind=jnp.bfloat16):
    array = spread * jax.random.normal(stream_key, extent, jnp.float32)
    if pieces:
        array = array * block_levels(stream_key, extent, pieces, -0.22, 0.18)
    return jnp.clip(array, -reach, reach).astype(kind)


def setup_inputs(seed: int = 0) -> dict:
    key_of = jax.random.split(jax.random.key(seed), 9)
    node_feats = noise(key_of[0], (NODES, H), 1.0, 6.0, ((0, 8), (1, 16)))
    rel_weight = noise(key_of[1], (R, H, H), H ** -0.5, 0.25)
    self_weight = noise(key_of[2], (H, H), H ** -0.5, 0.25)
    bias = noise(key_of[3], (H,), 0.5, 3.0, (), jnp.float32)
    out_degree = touch_ends(jax.random.randint(key_of[4], (R, NODES), 0, 64), jax.random.fold_in(key_of[4], 1), 0, 63).astype(jnp.int32)
    adjacency = touch_ends((jax.random.randint(key_of[5], (N_DOM, N_FEAT, TILE_DEV, TILE_SIZE, TILE_SIZE), 0, 8) < 1).astype(jnp.int32), jax.random.fold_in(key_of[5], 1), 0, 1)
    tile_index = draw_tile_index(jax.random.fold_in(key_of[8], 71), 0)
    tile_count = draw_tile_count(jax.random.fold_in(key_of[8], 71), 0)
    return dict(node_feats=node_feats, rel_weight=rel_weight, self_weight=self_weight, bias=bias, out_degree=out_degree, adjacency=adjacency, tile_index=tile_index, tile_count=tile_count)


def reference(node_feats, rel_weight, self_weight, bias, out_degree, adjacency, tile_index, tile_count):
    inv_degree = 1.0 / jnp.maximum(out_degree, 1).astype(jnp.float32)

    def transform(relation):
        product = jnp.dot(node_feats, rel_weight[relation], preferred_element_type=jnp.float32)
        return (product * inv_degree[relation][:, None]).astype(jnp.bfloat16)

    messages = lax.map(transform, jnp.arange(R, dtype=jnp.int32))
    flat_tiles = adjacency.reshape(-1, TILE_SIZE, TILE_SIZE)
    flat_index = tile_index.reshape(-1, 3).astype(jnp.int32)
    slot_ids = jnp.arange(TILE_DEV, dtype=jnp.int32)
    live_mask = (slot_ids[None, None, :] < tile_count[:, :, None]).reshape(-1).astype(jnp.float32)
    group_ids = jnp.repeat(jnp.arange(N_DOM, dtype=jnp.int32), N_FEAT * TILE_DEV)

    def accumulate(running, items):
        tile_cells, entry, weight, group = items
        source_row = ((group * BG + entry[2]) * TILE_SIZE).astype(jnp.int32)
        target_row = (entry[1] * TILE_SIZE).astype(jnp.int32)
        source_msg = lax.dynamic_slice(messages, (entry[0].astype(jnp.int32), source_row, jnp.int32(0)), (1, TILE_SIZE, H))[0]
        contribution = jnp.dot(tile_cells.astype(jnp.bfloat16), source_msg, preferred_element_type=jnp.float32) * weight
        current = lax.dynamic_slice_in_dim(running, target_row, TILE_SIZE, 0)
        return lax.dynamic_update_slice_in_dim(running, current + contribution, target_row, 0), None

    start = jnp.zeros((NODES, H), jnp.float32)
    aggregate, unused = lax.scan(accumulate, start, (flat_tiles, flat_index, live_mask, group_ids))
    self_term = jnp.dot(node_feats, self_weight, preferred_element_type=jnp.float32)
    return (aggregate + self_term + bias[None, :]).astype(jnp.bfloat16)
```

```python
import functools

import jax
import jax.numpy as jnp
from jax import lax
from jax.experimental import pallas as pl
from jax.experimental.pallas import tpu as pltpu
from jax.sharding import PartitionSpec as P

MESH = pl.DeviceIdType.MESH
BF = jnp.bfloat16
F32 = jnp.float32
RING = 4
HID = 512
COLS = 32
OWN = 1024
TILE = 256
SLOTS = 64
REL = 4
GROUPS = 8
BLOCKS = 32
LANES = (384, 384, 256)
VMEM = pl.BlockSpec(memory_space=pltpu.VMEM)
SMEM = pl.BlockSpec(memory_space=pltpu.SMEM)
HBM = pl.BlockSpec(memory_space=pl.ANY)
NT = (((1,), (1,)), ((), ()))


def place():
    dom = lax.axis_index("dom")
    feat = lax.axis_index("feat")
    return dict(z=dom // 2, c=dom % 2, x=feat // RING, y=feat % RING)


def device(here, **moved):
    at = dict(here)
    for axis, step in moved.items():
        at[axis] = (at[axis] + step) % (2 if axis == "c" else RING)
    return (at["z"] * 2 + at["c"], at["x"] * RING + at["y"])


def greet(peers):
    barrier = pltpu.get_barrier_semaphore()
    for peer in peers:
        pl.semaphore_signal(barrier, inc=1, device_id=peer, device_id_type=MESH)
    pl.semaphore_wait(barrier, len(peers))


def messages_kernel(
    nodes, rel, own, bias, degree, msg, self_term,
    feats, rel_in, own_in, rel_t, own_t, bias_t, send, recv, local,
):
    here = place()
    fetch_rel = pltpu.make_async_copy(rel, rel_in, local.at[0])
    fetch_own = pltpu.make_async_copy(own, own_in, local.at[1])
    fetch_rel.start()
    fetch_own.start()
    peers = [device(here, **{axis: step}) for axis in "xy" for step in (1, 2, 3)]
    greet(peers)
    half = COLS // 2
    first_axis = ("x", "y")
    second_axis = ("y", "x")

    def rows(h, x, y):
        return pl.ds(pl.multiple_of((x * RING + y) * COLS + h * half, half), half)

    def chunk(h, a, b):
        moved = {first_axis[h]: a, second_axis[h]: b}
        return rows(h, (here["x"] + moved["x"]) % RING, (here["y"] + moved["y"]) % RING)

    count = [0]
    started = []

    def remote(src, dst, peer):
        i = count[0]
        count[0] += 1
        copy = pltpu.make_async_remote_copy(
            src_ref=src, dst_ref=dst, send_sem=send.at[i], recv_sem=recv.at[i],
            device_id=peer, device_id_type=MESH,
        )
        return copy

    feats[rows(0, here["x"], here["y"]), :] = nodes[pl.ds(0, half), :]
    feats[rows(1, here["x"], here["y"]), :] = nodes[pl.ds(half, half), :]
    first = {}
    second = {}
    relay = {}
    left = pl.ds(0, OWN // 2)
    right = pl.ds(OWN // 2, OWN // 2)

    def part(h, a, b, lanes=None):
        at = chunk(h, a, b)
        return feats.at[at, :] if lanes is None else feats.at[at, lanes]

    for h in (0, 1):
        for step in (1, 3, 2):
            src = nodes.at[pl.ds(h * half, half), :]
            first[h, step] = remote(src, part(h, 0, 0), device(here, **{first_axis[h]: step}))
        for step in (1, 3):
            src = nodes.at[pl.ds(h * half, half), :]
            second[h, 0, step] = remote(src, part(h, 0, 0), device(here, **{second_axis[h]: step}))
        for a in (1, 3, 2):
            for step in (1, 3):
                second[h, a, step] = remote(
                    part(h, a, 0), part(h, a, 0), device(here, **{second_axis[h]: step})
                )
        for a in (0, 1, 3, 2):
            relay[h, a, 1] = remote(
                part(h, a, 3, left), part(h, a, 3, left), device(here, **{second_axis[h]: 1})
            )
            relay[h, a, 3] = remote(
                part(h, a, 1, right), part(h, a, 1, right), device(here, **{second_axis[h]: 3})
            )
    for step in (1, 3, 2):
        for h in (0, 1):
            first[h, step].start()
    for step in (1, 3):
        for h in (0, 1):
            second[h, 0, step].start()

    fetch_rel.wait()
    fetch_own.wait()
    rel_t[0] = rel_in[0].T
    for a in (3, 1):
        for h in (0, 1):
            first[h, RING - a].wait_recv()
            second[h, a, 1].start()
            second[h, a, 3].start()
    rel_t[1] = rel_in[1].T
    for h in (0, 1):
        second[h, 0, 1].wait_recv()
        relay[h, 0, 1].start()
        second[h, 0, 3].wait_recv()
        relay[h, 0, 3].start()
    for h in (0, 1):
        first[h, 2].wait_recv()
        second[h, 2, 1].start()
        second[h, 2, 3].start()
    rel_t[2] = rel_in[2].T
    for a in (3, 1):
        for h in (0, 1):
            second[h, a, 1].wait_recv()
            relay[h, a, 1].start()
            second[h, a, 3].wait_recv()
            relay[h, a, 3].start()
    rel_t[3] = rel_in[3].T
    for h in (0, 1):
        second[h, 2, 1].wait_recv()
        relay[h, 2, 1].start()
        second[h, 2, 3].wait_recv()
        relay[h, 2, 3].start()
    own_t[...] = own_in[...].T
    bias_t[...] = jnp.broadcast_to(bias[...], (128, HID)).T
    for a in (0, 3, 1, 2):
        for h in (0, 1):
            relay[h, a, 1].wait_recv()
            relay[h, a, 3].wait_recv()

    mine = pl.ds(pl.multiple_of((here["x"] * RING + here["y"]) * COLS, COLS), COLS)
    own_rows = own_t[mine, :]
    bias_rows = bias_t[mine, :]
    for s in range(OWN // TILE):
        at = pl.ds(s * TILE, TILE)
        block = feats[:, at]
        self_term[:, at] = (
            jnp.dot(own_rows, block, preferred_element_type=F32)
            + jnp.concatenate([bias_rows, bias_rows], axis=1)
        )

        def relation(r, carry):
            product = jnp.dot(rel_t[r], block, preferred_element_type=F32)
            factor = 1.0 / jnp.maximum(degree[pl.ds(r, 1), at], 1).astype(F32)
            msg[r * 4 + s] = (product * factor).astype(BF)
            return carry

        lax.fori_loop(0, REL, relation, 0)
    for copies in (first, second, relay):
        for copy in copies.values():
            copy.wait_send()


def messages(nodes, rel, own, bias, degree):
    copies = 2 * (3 + 8 + 8)
    return pl.pallas_call(
        messages_kernel,
        out_shape=(
            jax.ShapeDtypeStruct((REL * 4, HID, TILE), BF),
            jax.ShapeDtypeStruct((COLS, OWN), F32),
        ),
        in_specs=[VMEM, HBM, HBM, VMEM, VMEM],
        out_specs=(VMEM, VMEM),
        scratch_shapes=[
            pltpu.VMEM((HID, OWN), BF),
            pltpu.VMEM((REL, HID, HID), BF),
            pltpu.VMEM((HID, HID), BF),
            pltpu.VMEM((REL, HID, HID), BF),
            pltpu.VMEM((HID, HID), BF),
            pltpu.VMEM((HID, 128), F32),
            pltpu.SemaphoreType.DMA((copies,)),
            pltpu.SemaphoreType.DMA((copies,)),
            pltpu.SemaphoreType.DMA((2,)),
        ],
        compiler_params=pltpu.CompilerParams(collective_id=0, has_side_effects=True),
        name="messages",
    )(nodes, rel, own, bias, degree)


def tiles_kernel(index, live, msg, tiles, part_x, part_y, part_z, cells, total, arrived):
    parts = (part_x, part_y, part_z)
    count = live[0]

    def fetch(k):
        return pltpu.make_async_copy(tiles.at[k], cells.at[k], arrived.at[k])

    def start(k, carry):
        fetch(k).start()
        return carry

    lax.fori_loop(0, count, start, 0)

    def clear(d, carry):
        total[d] = jnp.zeros((HID, TILE), F32)
        return carry

    lax.fori_loop(0, BLOCKS, clear, 0)

    def add(k, carry):
        relation = index[0, k]
        target = index[1, k]
        source = index[2, k]
        fetch(k).wait()
        total[target] += lax.dot_general(
            msg[relation * 4 + source], cells[k].astype(F32).astype(BF), NT, preferred_element_type=F32
        )
        return carry

    lax.fori_loop(0, count, add, 0)

    def store(i, carry):
        f = i % 16
        g = i // 16
        x, y = f // RING, f % RING
        z, c = g // 2, g % 2
        at = pl.ds(pl.multiple_of(f * COLS, COLS), COLS)
        block = [total[g * 4 + b, at, :].astype(BF) for b in range(4)]
        part_x[c, x, y, z, :, 0:256] = block[0]
        part_x[c, x, y, z, :, 256:384] = block[1][:, 0:128]
        part_y[c, y, z, x, :, 0:128] = block[1][:, 128:256]
        part_y[c, y, z, x, :, 128:384] = block[2]
        part_z[c, z, x, y, :, :] = block[3]
        return carry

    lax.fori_loop(0, GROUPS * 16, store, 0)


def tile_sums(index, live, msg, tiles):
    return pl.pallas_call(
        tiles_kernel,
        out_shape=tuple(
            jax.ShapeDtypeStruct((2, RING, RING, RING, COLS, lanes), BF) for lanes in LANES
        ),
        in_specs=[SMEM, SMEM, VMEM, HBM],
        out_specs=(VMEM,) * 3,
        scratch_shapes=[
            pltpu.VMEM((SLOTS, TILE, TILE), jnp.int32),
            pltpu.VMEM((BLOCKS, HID, TILE), F32),
            pltpu.SemaphoreType.DMA((SLOTS,)),
        ],
        compiler_params=pltpu.CompilerParams(vmem_limit_bytes=60 * 2**20),
        name="tile_sums",
    )(index, live, msg, tiles)


ORDER = ("xyz", "yzx", "zxy")


def reduce_kernel(
    part_x, part_y, part_z, self_term, out,
    q1x, q1y, q1z, pair_x, pair_y, pair_z,
    relay1x, relay1y, relay1z, got1x, got1y, got1z,
    q2x, q2y, q2z, relay2x, relay2y, relay2z, got2x, got2y, got2z,
    q3x, q3y, q3z, relay3x, relay3y, relay3z, got3x, got3y, got3z,
    send, recv, pair_send, pair_recv, local,
):
    here = place()
    parts = (part_x, part_y, part_z)
    pair = (pair_x, pair_y, pair_z)
    held = ((q1x, q1y, q1z), (q2x, q2y, q2z), (q3x, q3y, q3z))
    relay = ((relay1x, relay1y, relay1z), (relay2x, relay2y, relay2z), (relay3x, relay3y, relay3z))
    got = ((got1x, got1y, got1z), (got2x, got2y, got2z), (got3x, got3y, got3z))
    c = here["c"]
    partner = device(here, c=1)

    def owner(p, stage, step):
        return (here[ORDER[p][stage]] + step) % RING

    steps = (2, 1, 3, 0)
    pair_copies = {}
    local_copies = {}
    for n, step in enumerate(steps):
        for p in range(3):
            i = n * 3 + p
            a = owner(p, 0, step)
            local_copies[p, step] = pltpu.make_async_copy(
                parts[p].at[c, a], held[0][p].at[a], local.at[i]
            )
            pair_copies[p, step] = pltpu.make_async_remote_copy(
                src_ref=parts[p].at[1 - c, a], dst_ref=pair[p].at[a],
                send_sem=pair_send.at[i], recv_sem=pair_recv.at[i],
                device_id=partner, device_id_type=MESH,
            )
    for copy in local_copies.values():
        copy.start()
    greet([partner] + [device(here, **{axis: step}) for axis in "xyz" for step in (1, 3)])
    for copy in pair_copies.values():
        copy.start()

    def half(ref, stage, index, which):
        n = ref.shape[1] // 2
        return ref.at[index, pl.ds(which * n, n)]

    def half_of(ref, index, which):
        n = ref.shape[1] // 2
        return ref.at[index, pl.ds(which * n, n)]

    copies = {}
    count = 0
    for stage in range(3):
        for p in range(3):
            axis = ORDER[p][stage]
            source = held[stage][p]
            lead = (source.shape[1] // 2,)

            def remote(src, dst, step):
                nonlocal count
                i = count
                count += 1
                return pltpu.make_async_remote_copy(
                    src_ref=src, dst_ref=dst, send_sem=send.at[i], recv_sem=recv.at[i],
                    device_id=device(here, **{axis: step}), device_id_type=MESH,
                )

            opposite = owner(p, stage, 2)
            after, before = owner(p, stage, 1), owner(p, stage, 3)
            copies[stage, p] = dict(
                relay_a=remote(half_of(source, opposite, 0), relay[stage][p].at[0], 1),
                relay_b=remote(half_of(source, opposite, 1), relay[stage][p].at[1], 3),
                direct_after=remote(half_of(source, after, 1), half_of(got[stage][p], 0, 1), 1),
                direct_before=remote(half_of(source, before, 0), half_of(got[stage][p], 1, 0), 3),
                summed_after=remote(half_of(source, after, 0), half_of(got[stage][p], 0, 0), 1),
                summed_before=remote(half_of(source, before, 1), half_of(got[stage][p], 1, 1), 3),
            )

    def add_blocks(dst, sources, shape):
        total = 1
        for n in shape[:-2]:
            total *= n

        def one(i, carry):
            at = []
            rest = i
            for n in reversed(shape[:-2]):
                at.append(rest % n)
                rest = rest // n
            at = tuple(reversed(at))
            value = sources[0][at].astype(F32)
            for source in sources[1:]:
                value += source[at].astype(F32)
            dst[at] = value.astype(dst.dtype)
            return carry

        if total == 1:
            one(0, 0)
        else:
            lax.fori_loop(0, total, one, 0)

    for step in steps:
        for p in range(3):
            a = owner(p, 0, step)
            local_copies[p, step].wait()
            pair_copies[p, step].wait_recv()
            q = held[0][p].at[a]
            add_blocks(q, (q, pair[p].at[a]), q.shape)
            if step == 2:
                copies[0, p]["relay_a"].start()
                copies[0, p]["relay_b"].start()
            elif step == 1:
                copies[0, p]["direct_after"].start()
            elif step == 3:
                copies[0, p]["direct_before"].start()
    for stage in range(3):
        if stage > 0:
            for p in range(3):
                for name in ("relay_a", "relay_b", "direct_after", "direct_before"):
                    copies[stage, p][name].start()
        for p in range(3):
            source = held[stage][p]
            after, before = owner(p, stage, 1), owner(p, stage, 3)
            copies[stage, p]["relay_a"].wait_recv()
            mine = half_of(source, after, 0)
            add_blocks(mine, (mine, relay[stage][p].at[0]), mine.shape)
            copies[stage, p]["summed_after"].start()
            copies[stage, p]["relay_b"].wait_recv()
            mine = half_of(source, before, 1)
            add_blocks(mine, (mine, relay[stage][p].at[1]), mine.shape)
            copies[stage, p]["summed_before"].start()
        start = 0
        for p in range(3):
            for name in ("direct_after", "direct_before", "summed_after", "summed_before"):
                copies[stage, p][name].wait_recv()
            mine = held[stage][p].at[owner(p, stage, 0)]
            arrived = got[stage][p]
            if stage < 2:
                into = held[stage + 1][p]
                add_blocks(into, (mine, arrived.at[0], arrived.at[1]), into.shape)
            else:
                lanes = pl.ds(start, LANES[p])
                out[:, lanes] = (
                    mine[...].astype(F32) + arrived[0].astype(F32) + arrived[1].astype(F32)
                    + self_term[:, lanes]
                ).astype(BF)
                start += LANES[p]
    for copy in pair_copies.values():
        copy.wait_send()
    for group in copies.values():
        for copy in group.values():
            copy.wait_send()


def reduced(parts, self_term):
    def buffers(*lead):
        return [pltpu.VMEM((*lead, COLS, lanes), BF) for lanes in LANES]

    last = [pltpu.VMEM((2, COLS // 2, lanes), BF) for lanes in LANES]
    copies = 3 * 3 * 6
    return pl.pallas_call(
        reduce_kernel,
        out_shape=jax.ShapeDtypeStruct((COLS, OWN), BF),
        in_specs=[HBM, HBM, HBM, VMEM],
        out_specs=VMEM,
        scratch_shapes=[
            *buffers(RING, RING, RING),
            *buffers(RING, RING, RING),
            *buffers(2, 2, RING),
            *buffers(2, RING, RING),
            *buffers(RING, RING),
            *buffers(2, 2),
            *buffers(2, RING),
            *buffers(RING),
            *last,
            *buffers(2),
            pltpu.SemaphoreType.DMA((copies,)),
            pltpu.SemaphoreType.DMA((copies,)),
            pltpu.SemaphoreType.DMA((12,)),
            pltpu.SemaphoreType.DMA((12,)),
            pltpu.SemaphoreType.DMA((12,)),
        ],
        compiler_params=pltpu.CompilerParams(collective_id=1, has_side_effects=True),
        name="reduce_to_owner",
    )(*parts, self_term)


def body(node_feats, rel_weight, self_weight, bias, out_degree, adjacency, tile_index, tile_count):
    msg, self_term = messages(
        node_feats.T, rel_weight, self_weight, bias.reshape(1, HID), out_degree
    )
    parts = tile_sums(tile_index[0, 0].T, tile_count.reshape(1), msg, adjacency[0, 0])
    return reduced(parts, self_term).T


def solution(mesh):
    placed = (
        P("dom", "feat"),
        P(),
        P(),
        P(),
        P(None, "dom"),
        P("dom", "feat", None, None, None),
        P("dom", "feat", None, None),
        P("dom", "feat"),
    )
    return jax.shard_map(
        body, mesh=mesh, in_specs=placed, out_specs=P("dom", "feat"), check_vma=False
    )
```

```python
import jax
import jax.numpy as jnp
from jax import lax
from jax.experimental import pallas as pl
from jax.experimental.pallas import tpu as pltpu
from jax.sharding import PartitionSpec as P

MESH = pl.DeviceIdType.MESH
BF = jnp.bfloat16
F32 = jnp.float32
I32 = jnp.int32
RING = 4
HID = 512
COLS = 32
ROWS = 16
OWN = 1024
TILE = 256
SLOTS = 64
REL = 4
BLOCKS = 32
HALVES = 2
BATCH = 4
DEPTH = 4
UNROLL = 8
LANES = (384, 384, 256)
ORDER = ("xyz", "yzx", "zxy")
STEPS = (2, 1, 3, 0)
VMEM = pl.BlockSpec(memory_space=pltpu.VMEM)
SMEM = pl.BlockSpec(memory_space=pltpu.SMEM)
HBM = pl.BlockSpec(memory_space=pl.ANY)
NT = (((1,), (1,)), ((), ()))
GATHER_COPIES = 2 * (3 + 8 + 8)
RING_COPIES = HALVES * 3 * 3 * 6
PAIR_COPIES = HALVES * 12


def place():
    dom = lax.axis_index("dom")
    feat = lax.axis_index("feat")
    return dict(z=dom // 2, c=dom % 2, x=feat // RING, y=feat % RING)


def device(here, **moved):
    at = dict(here)
    for axis, step in moved.items():
        at[axis] = (at[axis] + step) % (2 if axis == "c" else RING)
    return (at["z"] * 2 + at["c"], at["x"] * RING + at["y"])


def greet(peers):
    barrier = pltpu.get_barrier_semaphore()
    for peer in peers:
        pl.semaphore_signal(barrier, inc=1, device_id=peer, device_id_type=MESH)
    pl.semaphore_wait(barrier, len(peers))


def aligned(start, size):
    return pl.ds(pl.multiple_of(start, size), size)


def sort_slots(index, live, table):
    shape = (128, 128)
    across = lax.broadcasted_iota(I32, shape, 1)
    down = lax.broadcasted_iota(I32, shape, 0)

    def row(value):
        return jnp.broadcast_to(jnp.concatenate([value, value], axis=1), shape)

    is_live = across < live
    target = jnp.where(is_live, row(index[1]), BLOCKS)
    block = row(index[0]) * 4 + row(index[2])
    key = jnp.where(across < SLOTS, target * 128 + across, 65536 + across)
    key_down = key.T
    rank = jnp.sum(jnp.where(key_down < key, 1, 0), axis=0, keepdims=True)
    rank_down = jnp.broadcast_to(rank, shape).T
    hit = rank_down == across
    target_down = target.T
    table[0:1, :] = jnp.sum(jnp.where(hit, down, 0), axis=0, keepdims=True)
    table[1:2, :] = jnp.sum(jnp.where(hit, block.T, 0), axis=0, keepdims=True)
    table[2:3, :] = jnp.sum(jnp.where(hit, target_down, 0), axis=0, keepdims=True)
    real = down < SLOTS
    upto = jnp.sum(jnp.where(real & (target_down <= across), 1, 0), axis=0, keepdims=True)
    below = jnp.sum(jnp.where(real & (target_down < across), 1, 0), axis=0, keepdims=True)
    table[3:4, :] = jnp.where(upto > below, upto, 0)


def kernel(
    nodes, rel, own, bias, degree, index, live, tiles, out,
    feats, rel_in, own_in, rel_t, own_t, bias_t, self_term, inverse, msg,
    raw, cells, sums, table, order,
    out_x, out_y, out_z, pair_x, pair_y, pair_z,
    q1x, q1y, q1z, relay1x, relay1y, relay1z, got1x, got1y, got1z,
    q2x, q2y, q2z, relay2x, relay2y, relay2z, got2x, got2y, got2z,
    q3x, q3y, q3z, relay3x, relay3y, relay3z, got3x, got3y, got3z,
    gather_send, gather_recv, pair_send, pair_recv, ring_send, ring_recv, local, arrived,
):
    here = place()
    outgoing = (out_x, out_y, out_z)
    pair = (pair_x, pair_y, pair_z)
    held = ((q1x, q1y, q1z), (q2x, q2y, q2z), (q3x, q3y, q3z))
    relays = ((relay1x, relay1y, relay1z), (relay2x, relay2y, relay2z), (relay3x, relay3y, relay3z))
    gots = ((got1x, got1y, got1z), (got2x, got2y, got2z), (got3x, got3y, got3z))
    c = here["c"]

    fetch_rel = pltpu.make_async_copy(rel, rel_in, local.at[0])
    fetch_own = pltpu.make_async_copy(own, own_in, local.at[1])
    fetch_rel.start()
    fetch_own.start()

    def fetch_tiles(batch, slot):
        return pltpu.make_async_copy(
            tiles.at[pl.ds(batch * BATCH, BATCH)], raw.at[slot], arrived.at[slot]
        )

    for batch in range(DEPTH):
        fetch_tiles(batch, batch).start()
    partner = device(here, c=1)
    peers = [device(here, **{axis: step}) for axis in "xy" for step in (1, 2, 3)]
    peers += [device(here, z=step) for step in (1, 3)] + [partner]
    greet(peers)

    half = COLS // 2
    first_axis = ("x", "y")
    second_axis = ("y", "x")

    def rows(h, x, y):
        return aligned((x * RING + y) * COLS + h * half, half)

    counts = dict(gather=0, ring=0)

    def remote(src, dst, peer):
        i = counts["gather"]
        counts["gather"] += 1
        return pltpu.make_async_remote_copy(
            src_ref=src, dst_ref=dst, send_sem=gather_send.at[i], recv_sem=gather_recv.at[i],
            device_id=peer, device_id_type=MESH,
        )

    def part(h, a, b, lanes=pl.ds(0, OWN)):
        moved = {first_axis[h]: a, second_axis[h]: b}
        at = rows(h, (here["x"] + moved["x"]) % RING, (here["y"] + moved["y"]) % RING)
        return feats.at[at, lanes]

    for h in (0, 1):
        feats[rows(h, here["x"], here["y"]), :] = nodes[pl.ds(h * half, half), :]
    first, second, relay = {}, {}, {}
    left, right = pl.ds(0, OWN // 2), pl.ds(OWN // 2, OWN // 2)
    for h in (0, 1):
        src = nodes.at[pl.ds(h * half, half), :]
        for step in (1, 3, 2):
            first[h, step] = remote(src, part(h, 0, 0), device(here, **{first_axis[h]: step}))
        for a in (0, 1, 3, 2):
            for step in (1, 3):
                second[h, a, step] = remote(
                    src if a == 0 else part(h, a, 0), part(h, a, 0),
                    device(here, **{second_axis[h]: step}),
                )
            relay[h, a, 1] = remote(
                part(h, a, 3, left), part(h, a, 3, left), device(here, **{second_axis[h]: 1})
            )
            relay[h, a, 3] = remote(
                part(h, a, 1, right), part(h, a, 1, right), device(here, **{second_axis[h]: 3})
            )
    for step in (1, 3, 2):
        for h in (0, 1):
            first[h, step].start()
    for step in (1, 3):
        for h in (0, 1):
            second[h, 0, step].start()

    def transpose(r):
        turned = rel_in[r].T.reshape(HID // COLS, HALVES, ROWS, HID)
        for h in range(HALVES):
            rel_t[r, h] = turned[:, h].reshape(HID // 2, HID)

    def convert(low, high):
        def one(batch, carry):
            slot = batch % DEPTH
            fetch_tiles(batch, slot).wait()

            def tile(i, carry):
                cells[batch * BATCH + i] = raw[slot, i].astype(F32).astype(BF)
                return carry

            lax.fori_loop(0, BATCH, tile, 0, unroll=2)

            @pl.when(batch + DEPTH < SLOTS // BATCH)
            def _():
                fetch_tiles(batch + DEPTH, slot).start()

            return carry

        lax.fori_loop(low, high, one, 0)

    inverse[...] = 1.0 / jnp.maximum(degree[...], 1).astype(F32)
    sort_slots(index, live[0, 0], table)
    fetch_order = pltpu.make_async_copy(table, order, local.at[2])
    fetch_order.start()
    sums[0] = jnp.zeros((HID // 2, TILE), F32)
    fetch_rel.wait()
    fetch_own.wait()
    transpose(0)
    transpose(1)
    convert(0, 2)
    for a in (3, 1):
        for h in (0, 1):
            first[h, RING - a].wait_recv()
            second[h, a, 1].start()
            second[h, a, 3].start()
    transpose(2)
    for h in (0, 1):
        second[h, 0, 1].wait_recv()
        relay[h, 0, 1].start()
        second[h, 0, 3].wait_recv()
        relay[h, 0, 3].start()
    for h in (0, 1):
        first[h, 2].wait_recv()
        second[h, 2, 1].start()
        second[h, 2, 3].start()
    transpose(3)
    convert(2, 6)
    for a in (3, 1):
        for h in (0, 1):
            second[h, a, 1].wait_recv()
            relay[h, a, 1].start()
            second[h, a, 3].wait_recv()
            relay[h, a, 3].start()
    convert(6, 10)
    for h in (0, 1):
        second[h, 2, 1].wait_recv()
        relay[h, 2, 1].start()
        second[h, 2, 3].wait_recv()
        relay[h, 2, 3].start()
    own_t[...] = own_in[...].T
    bias_t[...] = jnp.broadcast_to(bias[...], (128, HID)).T
    convert(10, 16)
    fetch_order.wait()
    for a in (0, 3, 1, 2):
        for h in (0, 1):
            relay[h, a, 1].wait_recv()
            relay[h, a, 3].wait_recv()

    def make_messages(h):
        for s in range(OWN // TILE):
            at = pl.ds(s * TILE, TILE)

            def relation(r, carry):
                product = jnp.dot(rel_t[r, h], feats[:, at], preferred_element_type=F32)
                msg[h, r * 4 + s] = (product * inverse[pl.ds(r, 1), at]).astype(BF)
                return carry

            lax.fori_loop(0, REL, relation, 0, unroll=True)

    def make_self_term():
        mine = aligned((here["x"] * RING + here["y"]) * COLS, COLS)
        bias_rows = bias_t[mine, :]
        for s in range(OWN // TILE):
            at = pl.ds(s * TILE, TILE)
            self_term[:, at] = jnp.dot(
                own_t[mine, :], feats[:, at], preferred_element_type=F32
            ) + jnp.concatenate([bias_rows, bias_rows], axis=1)

    def add_tiles(h, low, high):
        def some(i, carry):
            for u in range(UNROLL):
                t = i * UNROLL + u
                product = lax.dot_general(
                    msg[h, order[1, t]], cells[order[0, t]], NT, preferred_element_type=F32
                )
                before = order[2, jnp.maximum(t - 1, 0)]
                same = jnp.where((t > 0) & (order[2, t] == before), 1.0, 0.0)
                sums[t + 1] = sums[t] * same + product
            return carry

        lax.fori_loop(low // UNROLL, high // UNROLL, some, 0)

    def owner(p, stage, step):
        return (here[ORDER[p][stage]] + step) % RING

    def build(p, h, a, core, dst):
        def one(i, carry):
            m, n = i // RING, i % RING
            if p == 0:
                x, y, z = a, m, n
            elif p == 1:
                x, y, z = n, a, m
            else:
                x, y, z = m, n, a
            at = aligned((x * RING + y) * ROWS, ROWS)
            base = z * 8 + core * 4
            if p == 0:
                dst[m, n, :, 0:256] = sums[order[3, base], at, :].astype(BF)
                dst[m, n, :, 256:384] = sums[order[3, base + 1], at, 0:128].astype(BF)
            elif p == 1:
                dst[m, n, :, 0:128] = sums[order[3, base + 1], at, 128:256].astype(BF)
                dst[m, n, :, 128:384] = sums[order[3, base + 2], at, :].astype(BF)
            else:
                dst[m, n] = sums[order[3, base + 3], at, :].astype(BF)
            return carry

        lax.fori_loop(0, RING * RING, one, 0, unroll=4)

    pair_copies = {}
    for h in range(HALVES):
        for n, step in enumerate(STEPS):
            for p in range(3):
                i = (h * 4 + n) * 3 + p
                a = owner(p, 0, step)
                pair_copies[h, p, step] = pltpu.make_async_remote_copy(
                    src_ref=outgoing[p].at[h, a], dst_ref=pair[p].at[h, a],
                    send_sem=pair_send.at[i], recv_sem=pair_recv.at[i],
                    device_id=partner, device_id_type=MESH,
                )

    def half_of(ref, lead, which):
        n = ref.shape[len(lead)] // 2
        return ref.at[(*lead, pl.ds(which * n, n))]

    ring = {}
    for h in range(HALVES):
        for stage in range(3):
            for p in range(3):
                axis = ORDER[p][stage]
                source, via, got = held[stage][p], relays[stage][p], gots[stage][p]

                def step_copy(src, dst, step):
                    i = counts["ring"]
                    counts["ring"] += 1
                    return pltpu.make_async_remote_copy(
                        src_ref=src, dst_ref=dst, send_sem=ring_send.at[i],
                        recv_sem=ring_recv.at[i],
                        device_id=device(here, **{axis: step}), device_id_type=MESH,
                    )

                opposite = owner(p, stage, 2)
                after, before = owner(p, stage, 1), owner(p, stage, 3)
                ring[h, stage, p] = dict(
                    relay_a=step_copy(half_of(source, (h, opposite), 0), via.at[h, 0], 1),
                    relay_b=step_copy(half_of(source, (h, opposite), 1), via.at[h, 1], 3),
                    direct_after=step_copy(
                        half_of(source, (h, after), 1), half_of(got, (h, 0), 1), 1
                    ),
                    direct_before=step_copy(
                        half_of(source, (h, before), 0), half_of(got, (h, 1), 0), 3
                    ),
                    summed_after=step_copy(
                        half_of(source, (h, after), 0), half_of(got, (h, 0), 0), 1
                    ),
                    summed_before=step_copy(
                        half_of(source, (h, before), 1), half_of(got, (h, 1), 1), 3
                    ),
                )

    def add_blocks(dst, sources):
        lead = dst.shape[:-3]
        total = 1
        for n in lead:
            total *= n

        def one(i, carry):
            at = []
            rest = i
            for n in reversed(lead):
                at.append(rest % n)
                rest = rest // n
            at = tuple(reversed(at))
            value = sources[0][at].astype(F32)
            for source in sources[1:]:
                value += source[at].astype(F32)
            dst[at] = value.astype(dst.dtype)
            return carry

        if total == 1:
            one(0, 0)
        else:
            lax.fori_loop(0, total, one, 0)

    def send_to_partner(h):
        for step in STEPS:
            for p in range(3):
                a = owner(p, 0, step)
                build(p, h, a, 1 - c, outgoing[p].at[h, a])
                pair_copies[h, p, step].start()

    def build_own(h):
        for step in STEPS:
            for p in range(3):
                a = owner(p, 0, step)
                build(p, h, a, c, held[0][p].at[h, a])

    def join_partner(h, step):
        for p in range(3):
            a = owner(p, 0, step)
            pair_copies[h, p, step].wait_recv()
            q = held[0][p].at[h, a]
            add_blocks(q, (q, pair[p].at[h, a]))
            if step == 2:
                ring[h, 0, p]["relay_a"].start()
                ring[h, 0, p]["relay_b"].start()
            elif step == 1:
                ring[h, 0, p]["direct_after"].start()
            elif step == 3:
                ring[h, 0, p]["direct_before"].start()

    def start_stage(h, stage):
        for p in range(3):
            for name in ("relay_a", "relay_b"):
                ring[h, stage, p][name].start()
        for p in range(3):
            for name in ("direct_after", "direct_before"):
                ring[h, stage, p][name].start()

    def pass_on(h, stage):
        for p in range(3):
            source, via, copies = held[stage][p], relays[stage][p], ring[h, stage, p]
            copies["relay_a"].wait_recv()
            mine = half_of(source, (h, owner(p, stage, 1)), 0)
            add_blocks(mine, (mine, via.at[h, 0])) if stage < 2 else add_flat(mine, via.at[h, 0])
            copies["summed_after"].start()
            copies["relay_b"].wait_recv()
            mine = half_of(source, (h, owner(p, stage, 3)), 1)
            add_blocks(mine, (mine, via.at[h, 1])) if stage < 2 else add_flat(mine, via.at[h, 1])
            copies["summed_before"].start()

    def add_flat(dst, other):
        dst[...] = dst[...] + other[...]

    def finish_stage(h, stage):
        start = 0
        for p in range(3):
            for name in ("direct_after", "direct_before", "summed_after", "summed_before"):
                ring[h, stage, p][name].wait_recv()
            mine = held[stage][p].at[h, owner(p, stage, 0)]
            got = gots[stage][p]
            if stage < 2:
                add_blocks(held[stage + 1][p].at[h], (mine, got.at[h, 0], got.at[h, 1]))
            else:
                at = pl.ds(h * ROWS, ROWS)
                lanes = pl.ds(start, LANES[p])
                out[at, lanes] = (
                    mine[...] + got[h, 0] + got[h, 1] + self_term[at, lanes]
                ).astype(BF)
                start += LANES[p]

    make_messages(0)
    add_tiles(0, 0, SLOTS)
    send_to_partner(0)
    build_own(0)
    join_partner(0, 2)
    make_messages(1)
    for step in (1, 3, 0):
        join_partner(0, step)
    add_tiles(1, 0, 40)
    pass_on(0, 0)
    add_tiles(1, 40, SLOTS)
    send_to_partner(1)
    build_own(1)
    join_partner(1, 2)
    finish_stage(0, 0)
    start_stage(0, 1)
    for step in (1, 3, 0):
        join_partner(1, step)
    make_self_term()
    pass_on(0, 1)
    pass_on(1, 0)
    finish_stage(0, 1)
    start_stage(0, 2)
    finish_stage(1, 0)
    start_stage(1, 1)
    pass_on(0, 2)
    pass_on(1, 1)
    finish_stage(0, 2)
    finish_stage(1, 1)
    start_stage(1, 2)
    pass_on(1, 2)
    finish_stage(1, 2)
    for copies in (first, second, relay, pair_copies):
        for copy in copies.values():
            copy.wait_send()
    for copies in ring.values():
        for copy in copies.values():
            copy.wait_send()


def body(node_feats, rel_weight, self_weight, bias, out_degree, adjacency, tile_index, tile_count):
    def buffers(*lead, kind=BF, rows=ROWS):
        return [pltpu.VMEM((HALVES, *lead, rows, lanes), kind) for lanes in LANES]

    result = pl.pallas_call(
        kernel,
        out_shape=jax.ShapeDtypeStruct((COLS, OWN), BF),
        in_specs=[VMEM, HBM, HBM, VMEM, VMEM, VMEM, SMEM, HBM],
        out_specs=VMEM,
        scratch_shapes=[
            pltpu.VMEM((HID, OWN), BF),
            pltpu.VMEM((REL, HID, HID), BF),
            pltpu.VMEM((HID, HID), BF),
            pltpu.VMEM((REL, HALVES, HID // 2, HID), BF),
            pltpu.VMEM((HID, HID), BF),
            pltpu.VMEM((HID, 128), F32),
            pltpu.VMEM((COLS, OWN), F32),
            pltpu.VMEM((REL, OWN), F32),
            pltpu.VMEM((HALVES, REL * 4, HID // 2, TILE), BF),
            pltpu.VMEM((DEPTH, BATCH, TILE, TILE), I32),
            pltpu.VMEM((SLOTS, TILE, TILE), BF),
            pltpu.VMEM((SLOTS + 1, HID // 2, TILE), F32),
            pltpu.VMEM((8, 128), I32),
            pltpu.SMEM((8, 128), I32),
            *buffers(RING, RING, RING),
            *buffers(RING, RING, RING),
            *buffers(RING, RING, RING),
            *buffers(2, 2, RING),
            *buffers(2, RING, RING),
            *buffers(RING, RING),
            *buffers(2, 2),
            *buffers(2, RING),
            *buffers(RING, kind=F32),
            *buffers(2, kind=F32, rows=ROWS // 2),
            *buffers(2, kind=F32),
            pltpu.SemaphoreType.DMA((GATHER_COPIES,)),
            pltpu.SemaphoreType.DMA((GATHER_COPIES,)),
            pltpu.SemaphoreType.DMA((PAIR_COPIES,)),
            pltpu.SemaphoreType.DMA((PAIR_COPIES,)),
            pltpu.SemaphoreType.DMA((RING_COPIES,)),
            pltpu.SemaphoreType.DMA((RING_COPIES,)),
            pltpu.SemaphoreType.DMA((3,)),
            pltpu.SemaphoreType.DMA((DEPTH,)),
        ],
        compiler_params=pltpu.CompilerParams(
            collective_id=0, has_side_effects=True, vmem_limit_bytes=63 * 2**20
        ),
        name="relational_layer",
    )(
        node_feats.T, rel_weight, self_weight, bias.reshape(1, HID), out_degree,
        jnp.transpose(tile_index[0], (2, 0, 1)), tile_count, adjacency[0, 0],
    )
    return result.T


def solution(mesh):
    placed = (
        P("dom", "feat"),
        P(),
        P(),
        P(),
        P(None, "dom"),
        P("dom", "feat", None, None, None),
        P("dom", "feat", None, None),
        P("dom", "feat"),
    )
    return jax.shard_map(
        body, mesh=mesh, in_specs=placed, out_specs=P("dom", "feat"), check_vma=False
    )
```

```python
import jax
import jax.numpy as jnp
from jax import lax
from jax.experimental import pallas as pl
from jax.experimental.pallas import tpu as pltpu
from jax.sharding import PartitionSpec as P

MESH = pl.DeviceIdType.MESH
BF = jnp.bfloat16
F32 = jnp.float32
I32 = jnp.int32
RING = 4
HID = 512
COLS = 32
ROWS = 16
OWN = 1024
TILE = 256
SLOTS = 64
REL = 4
BLOCKS = 32
HALVES = 2
BATCH = 4
DEPTH = 4
UNROLL = 8
LANES = (384, 384, 256)
ORDER = ("xyz", "yzx", "zxy")
STEPS = (2, 1, 3, 0)
DIRECT = (False, True, True)
VMEM = pl.BlockSpec(memory_space=pltpu.VMEM)
SMEM = pl.BlockSpec(memory_space=pltpu.SMEM)
HBM = pl.BlockSpec(memory_space=pl.ANY)
NT = (((1,), (1,)), ((), ()))
GATHER_ARRIVALS = 2 * (3 + 8) + 1
PAIR_ARRIVALS = HALVES * 12
RING_ARRIVALS = HALVES * 3 * sum(1 if direct else 3 for direct in DIRECT)


def place():
    dom = lax.axis_index("dom")
    feat = lax.axis_index("feat")
    return dict(z=dom // 2, c=dom % 2, x=feat // RING, y=feat % RING)


def device(here, **moved):
    at = dict(here)
    for axis, step in moved.items():
        at[axis] = (at[axis] + step) % (2 if axis == "c" else RING)
    return (at["z"] * 2 + at["c"], at["x"] * RING + at["y"])


def greet(peers):
    barrier = pltpu.get_barrier_semaphore()
    for peer in peers:
        pl.semaphore_signal(barrier, inc=1, device_id=peer, device_id_type=MESH)
    pl.semaphore_wait(barrier, len(peers))


def aligned(start, size):
    return pl.ds(pl.multiple_of(start, size), size)


def sort_slots(index, live, table):
    shape = (128, 128)
    across = lax.broadcasted_iota(I32, shape, 1)
    down = lax.broadcasted_iota(I32, shape, 0)

    def row(value):
        return jnp.broadcast_to(jnp.concatenate([value, value], axis=1), shape)

    is_live = across < live
    target = jnp.where(is_live, row(index[1]), BLOCKS)
    block = row(index[0]) * 4 + row(index[2])
    key = jnp.where(across < SLOTS, target * 128 + across, 65536 + across)
    key_down = key.T
    rank = jnp.sum(jnp.where(key_down < key, 1, 0), axis=0, keepdims=True)
    rank_down = jnp.broadcast_to(rank, shape).T
    hit = rank_down == across
    target_down = target.T
    table[0:1, :] = jnp.sum(jnp.where(hit, down, 0), axis=0, keepdims=True)
    table[1:2, :] = jnp.sum(jnp.where(hit, block.T, 0), axis=0, keepdims=True)
    table[2:3, :] = jnp.sum(jnp.where(hit, target_down, 0), axis=0, keepdims=True)
    real = down < SLOTS
    upto = jnp.sum(jnp.where(real & (target_down <= across), 1, 0), axis=0, keepdims=True)
    below = jnp.sum(jnp.where(real & (target_down < across), 1, 0), axis=0, keepdims=True)
    table[3:4, :] = jnp.where(upto > below, upto, 0)


def kernel(
    nodes, rel, own, bias, degree, index, live, tiles, result,
    out,    feats, rel_in, own_in, rel_t, own_t, bias_t, self_term, inverse, msg,
    raw, cells, sums, table, order,
    out_x, out_y, out_z, pair_x, pair_y, pair_z,
    q1x, q1y, q1z, relay1x, relay1y, relay1z, got1x, got1y, got1z,
    q2x, q2y, q2z, relay2x, relay2y, relay2z, got2x, got2y, got2z,
    q3x, q3y, q3z, relay3x, relay3y, relay3z, got3x, got3y, got3z,
    sent, gather_recv, pair_recv, ring_recv, local, arrived,
):
    here = place()
    outgoing = (out_x, out_y, out_z)
    pair = (pair_x, pair_y, pair_z)
    held = ((q1x, q1y, q1z), (q2x, q2y, q2z), (q3x, q3y, q3z))
    relays = ((relay1x, relay1y, relay1z), (relay2x, relay2y, relay2z), (relay3x, relay3y, relay3z))
    gots = ((got1x, got1y, got1z), (got2x, got2y, got2z), (got3x, got3y, got3z))
    c = here["c"]

    fetch_rel = pltpu.make_async_copy(rel, rel_in, local.at[0])
    fetch_own = pltpu.make_async_copy(own, own_in, local.at[1])
    fetch_rel.start()
    fetch_own.start()

    def fetch_tiles(batch, slot):
        return pltpu.make_async_copy(
            tiles.at[pl.ds(batch * BATCH, BATCH)], raw.at[slot], arrived.at[slot]
        )

    for batch in range(DEPTH):
        fetch_tiles(batch, batch).start()
    partner = device(here, c=1)
    peers = [device(here, **{axis: step}) for axis in "xy" for step in (1, 2, 3)]
    peers += [device(here, z=step) for step in (1, 3)] + [partner]
    greet(peers)

    half = COLS // 2
    first_axis = ("x", "y")
    second_axis = ("y", "x")

    def rows(h, x, y):
        return aligned((x * RING + y) * COLS + h * half, half)

    counts = dict(gather=0, ring=0)

    def remote(src, dst, peer, arrival=None):
        if arrival is None:
            arrival = counts["gather"]
            counts["gather"] += 1
        return pltpu.make_async_remote_copy(
            src_ref=src, dst_ref=dst, send_sem=sent.at[0], recv_sem=gather_recv.at[arrival],
            device_id=peer, device_id_type=MESH,
        )

    def part(h, a, b, lanes=pl.ds(0, OWN)):
        moved = {first_axis[h]: a, second_axis[h]: b}
        at = rows(h, (here["x"] + moved["x"]) % RING, (here["y"] + moved["y"]) % RING)
        return feats.at[at, lanes]

    for h in (0, 1):
        feats[rows(h, here["x"], here["y"]), :] = nodes[pl.ds(h * half, half), :]
    first, second, relay = {}, {}, {}
    left, right = pl.ds(0, OWN // 2), pl.ds(OWN // 2, OWN // 2)
    for h in (0, 1):
        src = nodes.at[pl.ds(h * half, half), :]
        for step in (1, 3, 2):
            first[h, step] = remote(src, part(h, 0, 0), device(here, **{first_axis[h]: step}))
        for a in (0, 1, 3, 2):
            for step in (1, 3):
                second[h, a, step] = remote(
                    src if a == 0 else part(h, a, 0), part(h, a, 0),
                    device(here, **{second_axis[h]: step}),
                )
            relay[h, a, 1] = remote(
                part(h, a, 3, left), part(h, a, 3, left), device(here, **{second_axis[h]: 1}),
                GATHER_ARRIVALS - 1,
            )
            relay[h, a, 3] = remote(
                part(h, a, 1, right), part(h, a, 1, right), device(here, **{second_axis[h]: 3}),
                GATHER_ARRIVALS - 1,
            )
    for step in (1, 3, 2):
        for h in (0, 1):
            first[h, step].start()
    for step in (1, 3):
        for h in (0, 1):
            second[h, 0, step].start()

    def transpose(r):
        turned = rel_in[r].T.reshape(HID // COLS, HALVES, ROWS, HID)
        for h in range(HALVES):
            rel_t[r, h] = turned[:, h].reshape(HID // 2, HID)

    def convert(low, high):
        def one(batch, carry):
            slot = batch % DEPTH
            fetch_tiles(batch, slot).wait()

            def tile(i, carry):
                cells[batch * BATCH + i] = raw[slot, i].astype(F32).astype(BF)
                return carry

            lax.fori_loop(0, BATCH, tile, 0, unroll=2)

            @pl.when(batch + DEPTH < SLOTS // BATCH)
            def _():
                fetch_tiles(batch + DEPTH, slot).start()

            return carry

        lax.fori_loop(low, high, one, 0)

    inverse[...] = 1.0 / jnp.maximum(degree[...], 1).astype(F32)
    sort_slots(index, live[0, 0], table)
    fetch_order = pltpu.make_async_copy(table, order, local.at[2])
    fetch_order.start()
    sums[0] = jnp.zeros((HID // 2, TILE), F32)
    fetch_rel.wait()
    fetch_own.wait()
    transpose(0)
    transpose(1)
    convert(0, 2)
    for a in (3, 1):
        for h in (0, 1):
            first[h, RING - a].wait_recv()
            second[h, a, 1].start()
            second[h, a, 3].start()
    transpose(2)
    for h in (0, 1):
        second[h, 0, 1].wait_recv()
        relay[h, 0, 1].start()
        second[h, 0, 3].wait_recv()
        relay[h, 0, 3].start()
    for h in (0, 1):
        first[h, 2].wait_recv()
        second[h, 2, 1].start()
        second[h, 2, 3].start()
    transpose(3)
    convert(2, 6)
    for a in (3, 1):
        for h in (0, 1):
            second[h, a, 1].wait_recv()
            relay[h, a, 1].start()
            second[h, a, 3].wait_recv()
            relay[h, a, 3].start()
    convert(6, 10)
    for h in (0, 1):
        second[h, 2, 1].wait_recv()
        relay[h, 2, 1].start()
        second[h, 2, 3].wait_recv()
        relay[h, 2, 3].start()
    own_t[...] = own_in[...].T
    bias_t[...] = jnp.broadcast_to(bias[...], (128, HID)).T
    convert(10, 16)
    fetch_order.wait()
    pltpu.make_async_copy(
        feats.at[pl.ds(0, 128)], feats.at[pl.ds(0, 128)], gather_recv.at[GATHER_ARRIVALS - 1]
    ).wait()

    def make_messages(h):
        for s in range(OWN // TILE):
            at = pl.ds(s * TILE, TILE)

            def relation(r, carry):
                product = jnp.dot(rel_t[r, h], feats[:, at], preferred_element_type=F32)
                msg[h, r * 4 + s] = (product * inverse[pl.ds(r, 1), at]).astype(BF)
                return carry

            lax.fori_loop(0, REL, relation, 0, unroll=True)

    def make_self_term():
        mine = aligned((here["x"] * RING + here["y"]) * COLS, COLS)
        bias_rows = bias_t[mine, :]
        for s in range(OWN // TILE):
            at = pl.ds(s * TILE, TILE)
            self_term[:, at] = jnp.dot(
                own_t[mine, :], feats[:, at], preferred_element_type=F32
            ) + jnp.concatenate([bias_rows, bias_rows], axis=1)

    def add_tiles(h, low, high):
        def some(i, carry):
            for u in range(UNROLL):
                t = i * UNROLL + u
                product = lax.dot_general(
                    msg[h, order[1, t]], cells[order[0, t]], NT, preferred_element_type=F32
                )
                before = order[2, jnp.maximum(t - 1, 0)]
                same = jnp.where((t > 0) & (order[2, t] == before), 1.0, 0.0)
                sums[t + 1] = sums[t] * same + product
            return carry

        lax.fori_loop(low // UNROLL, high // UNROLL, some, 0)

    def owner(p, stage, step):
        return (here[ORDER[p][stage]] + step) % RING

    def own_blocks(p, a, core, i):
        if p == 0:
            at = aligned(a * RING * ROWS, RING * ROWS)
            base = i * 8 + core * 4
            shape = (RING, ROWS, -1)
            yield (slice(None), i, slice(None), pl.ds(0, 256)), sums[order[3, base], at, :].reshape(
                RING, ROWS, 256
            )
            yield (slice(None), i, slice(None), pl.ds(256, 128)), sums[
                order[3, base + 1], at, 0:128
            ].reshape(RING, ROWS, 128)
        elif p == 1:
            base = i * 8 + core * 4
            for x in range(RING):
                at = aligned((x * RING + a) * ROWS, ROWS)
                yield (i, x, slice(None), pl.ds(0, 128)), sums[order[3, base + 1], at, 128:256]
                yield (i, x, slice(None), pl.ds(128, 256)), sums[order[3, base + 2], at, :]
        else:
            at = aligned(i * RING * ROWS, RING * ROWS)
            base = a * 8 + core * 4
            yield (i,), sums[order[3, base + 3], at, :].reshape(RING, ROWS, 256)

    def build(p, a, core, dst):
        def one(i, carry):
            for at, value in own_blocks(p, a, core, i):
                dst[at] = value.astype(BF)
            return carry

        lax.fori_loop(0, RING, one, 0, unroll=True)

    def build_joined(p, a, core, dst, other):
        def one(i, carry):
            for at, value in own_blocks(p, a, core, i):
                dst[at] = (value + other[at].astype(F32)).astype(BF)
            return carry

        lax.fori_loop(0, RING, one, 0, unroll=True)

    pair_copies = {}
    for h in range(HALVES):
        for n, step in enumerate(STEPS):
            for p in range(3):
                i = (h * 4 + n) * 3 + p
                a = owner(p, 0, step)
                pair_copies[h, p, step] = pltpu.make_async_remote_copy(
                    src_ref=outgoing[p].at[h, a], dst_ref=pair[p].at[h, a],
                    send_sem=sent.at[1 + p], recv_sem=pair_recv.at[i],
                    device_id=partner, device_id_type=MESH,
                )

    def half_of(ref, lead, which):
        n = ref.shape[len(lead)] // 2
        return ref.at[(*lead, pl.ds(which * n, n))]

    ring = {}
    for h in range(HALVES):
        for stage in range(3):
            for p in range(3):
                axis = ORDER[p][stage]
                source, via, got = held[stage][p], relays[stage][p], gots[stage][p]

                joint = counts["ring"]
                counts["ring"] += 1

                def step_copy(src, dst, step, alone=False):
                    arrival = joint
                    if alone:
                        arrival = counts["ring"]
                        counts["ring"] += 1
                    return pltpu.make_async_remote_copy(
                        src_ref=src, dst_ref=dst, send_sem=sent.at[4 + stage * 3 + p],
                        recv_sem=ring_recv.at[arrival],
                        device_id=device(here, **{axis: step}), device_id_type=MESH,
                    )

                opposite = owner(p, stage, 2)
                after, before = owner(p, stage, 1), owner(p, stage, 3)
                if DIRECT[stage]:
                    ring[h, stage, p] = dict(
                        joint=joint,
                        opposite=step_copy(source.at[h, opposite], got.at[h, 2], 2),
                        after=step_copy(source.at[h, after], got.at[h, 0], 1),
                        before=step_copy(source.at[h, before], got.at[h, 1], 3),
                    )
                    continue
                ring[h, stage, p] = dict(
                    joint=joint,
                    relay_a=step_copy(half_of(source, (h, opposite), 0), via.at[h, 0], 1, True),
                    relay_b=step_copy(half_of(source, (h, opposite), 1), via.at[h, 1], 3, True),
                    direct_after=step_copy(
                        half_of(source, (h, after), 1), half_of(got, (h, 0), 1), 1
                    ),
                    direct_before=step_copy(
                        half_of(source, (h, before), 0), half_of(got, (h, 1), 0), 3
                    ),
                    summed_after=step_copy(
                        half_of(source, (h, after), 0), half_of(got, (h, 0), 0), 1
                    ),
                    summed_before=step_copy(
                        half_of(source, (h, before), 1), half_of(got, (h, 1), 1), 3
                    ),
                )

    def add_blocks(dst, sources):
        lead = dst.shape[:-3]
        total = 1
        for n in lead:
            total *= n

        def one(i, carry):
            at = []
            rest = i
            for n in reversed(lead):
                at.append(rest % n)
                rest = rest // n
            at = tuple(reversed(at))
            value = sources[0][at].astype(F32)
            for source in sources[1:]:
                value += source[at].astype(F32)
            dst[at] = value.astype(dst.dtype)
            return carry

        if total == 1:
            one(0, 0)
        else:
            lax.fori_loop(0, total, one, 0)

    def send_to_partner(h):
        for step in STEPS:
            for p in range(3):
                a = owner(p, 0, step)
                build(p, a, 1 - c, outgoing[p].at[h, a])
                pair_copies[h, p, step].start()

    def join_partner(h, step):
        for p in range(3):
            a = owner(p, 0, step)
            pair_copies[h, p, step].wait_recv()
            build_joined(p, a, c, held[0][p].at[h, a], pair[p].at[h, a])
            if step == 2:
                ring[h, 0, p]["relay_a"].start()
                ring[h, 0, p]["relay_b"].start()
            elif step == 1:
                ring[h, 0, p]["direct_after"].start()
            elif step == 3:
                ring[h, 0, p]["direct_before"].start()

    def start_stage(h, stage):
        if DIRECT[stage]:
            for name in ("opposite", "after", "before"):
                for p in range(3):
                    ring[h, stage, p][name].start()
            return
        for p in range(3):
            for name in ("relay_a", "relay_b"):
                ring[h, stage, p][name].start()
        for p in range(3):
            for name in ("direct_after", "direct_before"):
                ring[h, stage, p][name].start()

    def pass_on(h, stage):
        if DIRECT[stage]:
            return
        for p in range(3):
            source, via, copies = held[stage][p], relays[stage][p], ring[h, stage, p]
            copies["relay_a"].wait_recv()
            mine = half_of(source, (h, owner(p, stage, 1)), 0)
            add_blocks(mine, (mine, via.at[h, 0])) if stage < 2 else add_flat(mine, via.at[h, 0])
            copies["summed_after"].start()
            copies["relay_b"].wait_recv()
            mine = half_of(source, (h, owner(p, stage, 3)), 1)
            add_blocks(mine, (mine, via.at[h, 1])) if stage < 2 else add_flat(mine, via.at[h, 1])
            copies["summed_before"].start()

    def add_flat(dst, other):
        dst[...] = dst[...] + other[...]

    def finish_stage(h, stage):
        start = 0
        for p in range(3):
            mine = held[stage][p].at[h, owner(p, stage, 0)]
            got = gots[stage][p]
            arrival = ring_recv.at[ring[h, stage, p]["joint"]]
            pltpu.make_async_copy(got.at[h], got.at[h], arrival).wait()
            arrivals = range(3 if DIRECT[stage] else 2)
            if stage < 2:
                add_blocks(held[stage + 1][p].at[h], (mine, *(got.at[h, i] for i in arrivals)))
            else:
                at = pl.ds(h * ROWS, ROWS)
                lanes = pl.ds(start, LANES[p])
                value = mine[...].astype(F32) + self_term[at, lanes]
                for i in arrivals:
                    value += got[h, i].astype(F32)
                out[at, lanes] = value.astype(BF)
                start += LANES[p]

    def wait_all_sent():
        pltpu.make_async_copy(feats.at[pl.ds(0, 480)], feats.at[pl.ds(0, 480)], sent.at[0]).wait()
        for p in range(3):
            whole = outgoing[p]
            pltpu.make_async_copy(whole, whole, sent.at[1 + p]).wait()
            for stage in range(3):
                whole = held[stage][p].at[:, pl.ds(0, RING - 1)]
                pltpu.make_async_copy(whole, whole, sent.at[4 + stage * 3 + p]).wait()

    make_messages(0)
    add_tiles(0, 0, SLOTS)
    send_to_partner(0)
    make_messages(1)
    join_partner(0, 2)
    make_self_term()
    for step in (1, 3, 0):
        join_partner(0, step)
    add_tiles(1, 0, 40)
    pass_on(0, 0)
    add_tiles(1, 40, SLOTS)
    send_to_partner(1)
    for step in STEPS:
        join_partner(1, step)
    finish_stage(0, 0)
    start_stage(0, 1)
    pass_on(0, 1)
    pass_on(1, 0)
    finish_stage(0, 1)
    start_stage(0, 2)
    finish_stage(1, 0)
    start_stage(1, 1)
    pass_on(0, 2)
    finish_stage(0, 2)
    pass_on(1, 1)
    finish_stage(1, 1)
    start_stage(1, 2)
    pass_on(1, 2)
    finish_stage(1, 2)
    store = pltpu.make_async_copy(out, result, local.at[2])
    store.start()
    wait_all_sent()
    store.wait()


def body(node_feats, rel_weight, self_weight, bias, out_degree, adjacency, tile_index, tile_count):
    def buffers(*lead, kind=BF, rows=ROWS):
        return [pltpu.VMEM((HALVES, *lead, rows, lanes), kind) for lanes in LANES]

    result = pl.pallas_call(
        kernel,
        out_shape=jax.ShapeDtypeStruct((COLS, OWN), BF),
        in_specs=[VMEM, HBM, HBM, VMEM, VMEM, VMEM, SMEM, HBM],
        out_specs=HBM,
        scratch_shapes=[
            pltpu.VMEM((COLS, OWN), BF),
            pltpu.VMEM((HID, OWN), BF),
            pltpu.VMEM((REL, HID, HID), BF),
            pltpu.VMEM((HID, HID), BF),
            pltpu.VMEM((REL, HALVES, HID // 2, HID), BF),
            pltpu.VMEM((HID, HID), BF),
            pltpu.VMEM((HID, 128), F32),
            pltpu.VMEM((COLS, OWN), F32),
            pltpu.VMEM((REL, OWN), F32),
            pltpu.VMEM((HALVES, REL * 4, HID // 2, TILE), BF),
            pltpu.VMEM((DEPTH, BATCH, TILE, TILE), I32),
            pltpu.VMEM((SLOTS, TILE, TILE), BF),
            pltpu.VMEM((SLOTS + 1, HID // 2, TILE), F32),
            pltpu.VMEM((8, 128), I32),
            pltpu.SMEM((8, 128), I32),
            *buffers(RING, RING, RING),
            *buffers(RING, RING, RING),
            *buffers(RING, RING, RING),
            *buffers(2, 2, RING),
            *buffers(2, RING, RING),
            *buffers(RING, RING),
            *buffers(2, 2),
            *buffers(3 if DIRECT[1] else 2, RING),
            *buffers(RING, kind=F32),
            *buffers(2, kind=F32, rows=ROWS // 2),
            *buffers(3 if DIRECT[2] else 2, kind=F32),
            pltpu.SemaphoreType.DMA((13,)),
            pltpu.SemaphoreType.DMA((GATHER_ARRIVALS,)),
            pltpu.SemaphoreType.DMA((PAIR_ARRIVALS,)),
            pltpu.SemaphoreType.DMA((RING_ARRIVALS,)),
            pltpu.SemaphoreType.DMA((3,)),
            pltpu.SemaphoreType.DMA((DEPTH,)),
        ],
        compiler_params=pltpu.CompilerParams(
            collective_id=0, has_side_effects=True, vmem_limit_bytes=63 * 2**20
        ),
        name="relational_layer",
    )(
        node_feats.T, rel_weight, self_weight, bias.reshape(1, HID), out_degree,
        jnp.transpose(tile_index[0], (2, 0, 1)), tile_count, adjacency[0, 0],
    )
    return result.T


def solution(mesh):
    placed = (
        P("dom", "feat"),
        P(),
        P(),
        P(),
        P(None, "dom"),
        P("dom", "feat", None, None, None),
        P("dom", "feat", None, None),
        P("dom", "feat"),
    )
    return jax.shard_map(
        body, mesh=mesh, in_specs=placed, out_specs=P("dom", "feat"), check_vma=False
    )
```

```python
import jax
import jax.numpy as jnp
from jax import lax
from jax.experimental import pallas as pl
from jax.experimental.pallas import tpu as pltpu
from jax.sharding import PartitionSpec as P

MESH = pl.DeviceIdType.MESH
BF = jnp.bfloat16
F32 = jnp.float32
I32 = jnp.int32
RING = 4
HID = 512
COLS = 32
ROWS = 8
OWN = 1024
TILE = 256
SLOTS = 64
REL = 4
BLOCKS = 32
HALVES = 2
PIECES = 4
BATCH = 4
DEPTH = 8
UNROLL = 32
LANES = (384, 384, 256)
ORDER = ("xyz", "yzx", "zxy")
STEPS = (2, 1, 3, 0)
VMEM = pl.BlockSpec(memory_space=pltpu.VMEM)
SMEM = pl.BlockSpec(memory_space=pltpu.SMEM)
HBM = pl.BlockSpec(memory_space=pl.ANY)
NT = (((1,), (1,)), ((), ()))
GATHER_ARRIVALS = 2 * 3 + 1
PAIR_ARRIVALS = PIECES * 4
RING_ARRIVALS = PIECES * 9


def place():
    dom = lax.axis_index("dom")
    feat = lax.axis_index("feat")
    return dict(z=dom // 2, c=dom % 2, x=feat // RING, y=feat % RING)


def device(here, **moved):
    at = dict(here)
    for axis, step in moved.items():
        at[axis] = (at[axis] + step) % (2 if axis == "c" else RING)
    return (at["z"] * 2 + at["c"], at["x"] * RING + at["y"])


def greet(peers):
    barrier = pltpu.get_barrier_semaphore()
    for peer in peers:
        pl.semaphore_signal(barrier, inc=1, device_id=peer, device_id_type=MESH)
    pl.semaphore_wait(barrier, len(peers))


def aligned(start, size):
    return pl.ds(pl.multiple_of(start, size), size)


def sort_slots(index, live, table):
    shape = (128, 128)
    across = lax.broadcasted_iota(I32, shape, 1)
    down = lax.broadcasted_iota(I32, shape, 0)

    def row(value):
        return jnp.broadcast_to(jnp.concatenate([value, value], axis=1), shape)

    is_live = across < live
    target = jnp.where(is_live, row(index[1]), BLOCKS)
    block = row(index[0]) * 4 + row(index[2])
    key = jnp.where(across < SLOTS, target * 128 + across, 65536 + across)
    key_down = key.T
    rank = jnp.sum(jnp.where(key_down < key, 1, 0), axis=0, keepdims=True)
    rank_down = jnp.broadcast_to(rank, shape).T
    hit = rank_down == across
    target_down = target.T
    table[0:1, :] = jnp.sum(jnp.where(hit, down, 0), axis=0, keepdims=True)
    table[1:2, :] = jnp.sum(jnp.where(hit, block.T, 0), axis=0, keepdims=True)
    table[2:3, :] = jnp.sum(jnp.where(hit, target_down, 0), axis=0, keepdims=True)
    real = down < SLOTS
    upto = jnp.sum(jnp.where(real & (target_down <= across), 1, 0), axis=0, keepdims=True)
    below = jnp.sum(jnp.where(real & (target_down < across), 1, 0), axis=0, keepdims=True)
    table[3:4, :] = jnp.where(upto > below, upto, 0)


def kernel(
    nodes, rel, own, bias_hbm, degree_hbm, index_hbm, live, tiles, result,
    bias, degree, index, out,    feats, rel_in, own_in, rel_t, own_t, bias_t, self_term, inverse, msg,
    raw, cells, sums, table, order,
    out_x, out_y, out_z, pair_x, pair_y, pair_z,
    relay_x, relay_y, relay_z, got1x, got1y, got1z,
    q2x, q2y, q2z, got2x, got2y, got2z, q3x, q3y, q3z, got3x, got3y, got3z,
    sent, gather_recv, pair_recv, ring_recv, local, arrived,
):
    here = place()
    outgoing = (out_x, out_y, out_z)
    pair = (pair_x, pair_y, pair_z)
    relays = (relay_x, relay_y, relay_z)
    got1, got2, got3 = (got1x, got1y, got1z), (got2x, got2y, got2z), (got3x, got3y, got3z)
    q2, q3 = (q2x, q2y, q2z), (q3x, q3y, q3z)
    c = here["c"]

    mine = aligned((here["x"] * RING + here["y"]) * COLS, COLS)
    fetch_nodes = pltpu.make_async_copy(nodes, feats.at[mine, :], local.at[3])
    fetch_nodes.start()
    fetch_small = [
        pltpu.make_async_copy(src, dst, local.at[4 + i])
        for i, (src, dst) in enumerate(((index_hbm, index), (degree_hbm, degree), (bias_hbm, bias)))
    ]
    for fetch in fetch_small:
        fetch.start()
    fetch_rel = pltpu.make_async_copy(rel, rel_in, local.at[0])
    fetch_own = pltpu.make_async_copy(own, own_in, local.at[1])
    fetch_rel.start()
    fetch_own.start()

    def fetch_tiles(batch, slot):
        return pltpu.make_async_copy(
            tiles.at[pl.ds(batch * BATCH, BATCH)], raw.at[slot], arrived.at[slot]
        )

    for batch in range(DEPTH):
        fetch_tiles(batch, batch).start()
    partner = device(here, c=1)
    peers = [device(here, **{axis: step}) for axis in "xy" for step in (1, 2, 3)]
    peers += [device(here, z=step) for step in (1, 3)] + [partner]
    greet(peers)

    half = COLS // 2
    first_axis = ("x", "y")
    second_axis = ("y", "x")

    def rows(h, x, y):
        return aligned((x * RING + y) * COLS + h * half, half)

    counts = dict(gather=0)

    def remote(src, dst, peer, arrival=None):
        if arrival is None:
            arrival = counts["gather"]
            counts["gather"] += 1
        return pltpu.make_async_remote_copy(
            src_ref=src, dst_ref=dst, send_sem=sent.at[0], recv_sem=gather_recv.at[arrival],
            device_id=peer, device_id_type=MESH,
        )

    def part(h, a, b, lanes=pl.ds(0, OWN)):
        moved = {first_axis[h]: a, second_axis[h]: b}
        at = rows(h, (here["x"] + moved["x"]) % RING, (here["y"] + moved["y"]) % RING)
        return feats.at[at, lanes]

    fetch_nodes.wait()
    first, second = {}, {}
    for h in (0, 1):
        src = part(h, 0, 0)
        for step in (1, 3, 2):
            first[h, step] = remote(src, part(h, 0, 0), device(here, **{first_axis[h]: step}))
        for a in (0, 1, 3, 2):
            for step in (1, 3, 2):
                second[h, a, step] = remote(
                    part(h, a, 0), part(h, a, 0),
                    device(here, **{second_axis[h]: step}), GATHER_ARRIVALS - 1,
                )
    for step in (1, 3, 2):
        for h in (0, 1):
            first[h, step].start()
    for step in (2, 1, 3):
        for h in (0, 1):
            second[h, 0, step].start()

    def forward(a):
        for h in (0, 1):
            first[h, RING - a].wait_recv()
            for step in (2, 1, 3):
                second[h, a, step].start()

    def transpose(r):
        turned = rel_in[r].astype(F32).T.reshape(HID // COLS, HALVES, 2, ROWS, HID)
        for h in range(HALVES):
            for i in range(2):
                some = turned[:, h, i].reshape(HID // PIECES, HID)
                rel_t[r, h, pl.ds(i * (HID // PIECES), HID // PIECES), :] = some.astype(BF)

    def convert(low, high):
        def one(batch, carry):
            slot = batch % DEPTH
            fetch_tiles(batch, slot).wait()

            def tile(i, carry):
                cells[batch * BATCH + i] = raw[slot, i].astype(F32).astype(BF)
                return carry

            lax.fori_loop(0, BATCH, tile, 0, unroll=2)

            @pl.when(batch + DEPTH < SLOTS // BATCH)
            def _():
                fetch_tiles(batch + DEPTH, slot).start()

            return carry

        lax.fori_loop(low, high, one, 0)

    for fetch in fetch_small:
        fetch.wait()
    inverse[...] = 1.0 / jnp.maximum(degree[...], 1).astype(F32)
    sort_slots(index, live[0, 0], table)
    fetch_order = pltpu.make_async_copy(table, order, local.at[2])
    fetch_order.start()
    sums[0] = jnp.zeros((HID // 2, TILE), F32)
    fetch_rel.wait()
    fetch_own.wait()
    for r in range(REL):
        transpose(r)
    convert(0, 6)
    forward(3)
    forward(1)
    forward(2)
    own_t[...] = own_in[...].T
    bias_t[...] = jnp.broadcast_to(bias[...], (128, HID)).T
    convert(6, SLOTS // BATCH)
    fetch_order.wait()
    rest = feats.at[pl.ds(0, 384)]
    pltpu.make_async_copy(rest, rest, gather_recv.at[GATHER_ARRIVALS - 1]).wait()

    def make_messages(h, sources):
        for s in sources:
            at = pl.ds(s * TILE, TILE)

            def relation(r, carry):
                product = jnp.dot(rel_t[r, h], feats[:, at], preferred_element_type=F32)
                msg[h, r * 4 + s] = (product * inverse[pl.ds(r, 1), at]).astype(BF)
                return carry

            lax.fori_loop(0, REL, relation, 0, unroll=True)

    def make_self_term():
        bias_rows = bias_t[mine, :]
        for s in range(OWN // TILE):
            at = pl.ds(s * TILE, TILE)
            self_term[:, at] = jnp.dot(
                own_t[mine, :], feats[:, at], preferred_element_type=F32
            ) + jnp.concatenate([bias_rows, bias_rows], axis=1)

    def add_tiles(h, low, high):
        def some(i, carry):
            for u in range(UNROLL):
                t = i * UNROLL + u
                product = lax.dot_general(
                    msg[h, order[1, t]], cells[order[0, t]], NT, preferred_element_type=F32
                )
                before = order[2, jnp.maximum(t - 1, 0)]
                same = jnp.where((t > 0) & (order[2, t] == before), 1.0, 0.0)
                sums[t + 1] = sums[t] * same + product
            return carry

        lax.fori_loop(low // UNROLL, high // UNROLL, some, 0)

    def owner(p, stage, step):
        return (here[ORDER[p][stage]] + step) % RING

    def blocks(k, p, a, core):
        start = k % 2 * (HID // PIECES)

        def at(x, y):
            return aligned(start + (x * RING + y) * ROWS, ROWS)

        def last(z, b):
            return order[3, z * 8 + core * 4 + b]

        if p == 2:
            for x in range(RING):
                rows = aligned(start + x * RING * ROWS, RING * ROWS)
                yield x, pl.ds(0, 256), sums[last(a, 3), rows, :]
            return
        for m in range(RING):
            if p == 0:
                one = [sums[last(z, 0), at(a, m), :] for z in range(RING)]
                two = [sums[last(z, 1), at(a, m), 0:128] for z in range(RING)]
            else:
                one = [sums[last(m, 1), at(x, a), 128:256] for x in range(RING)]
                two = [sums[last(m, 2), at(x, a), :] for x in range(RING)]
            width = one[0].shape[1]
            yield m, pl.ds(0, width), jnp.concatenate(one, axis=0)
            yield m, pl.ds(width, 384 - width), jnp.concatenate(two, axis=0)

    def await_bytes(ref, semaphore):
        pltpu.make_async_copy(ref, ref, semaphore).wait()

    pair_copies = {}
    for k in range(PIECES):
        for n, step in enumerate(STEPS):
            for p in range(3):
                a = owner(p, 0, step)
                pair_copies[k, p, step] = pltpu.make_async_remote_copy(
                    src_ref=outgoing[p].at[k, a], dst_ref=pair[p].at[k, a],
                    send_sem=sent.at[1], recv_sem=pair_recv.at[k * 4 + n],
                    device_id=partner, device_id_type=MESH,
                )

    def half_of(ref, lead, which):
        n = ref.shape[len(lead)] // 2
        return ref.at[(*lead, pl.ds(which * n, n))]

    ring = {}
    for k in range(PIECES):
        for p in range(3):

            def step_copy(stage, src, dst, step, arrival):
                return pltpu.make_async_remote_copy(
                    src_ref=src, dst_ref=dst, send_sem=sent.at[2 + stage],
                    recv_sem=ring_recv.at[k * 9 + arrival],
                    device_id=device(here, **{ORDER[p][stage]: step}), device_id_type=MESH,
                )

            opposite, after, before = (owner(p, 0, step) for step in (2, 1, 3))
            source, via, got = pair[p], relays[p], got1[p]
            ring[k, 0, p] = dict(
                relay_a=step_copy(0, half_of(source, (k, opposite), 0), via.at[k, 0], 1, 3 + p),
                relay_b=step_copy(0, half_of(source, (k, opposite), 1), via.at[k, 1], 3, 6 + p),
                direct_after=step_copy(
                    0, half_of(source, (k, after), 1), half_of(got, (k, 0), 1), 1, 0
                ),
                direct_before=step_copy(
                    0, half_of(source, (k, before), 0), half_of(got, (k, 1), 0), 3, 0
                ),
                summed_after=step_copy(
                    0, half_of(source, (k, after), 0), half_of(got, (k, 0), 0), 1, 0
                ),
                summed_before=step_copy(
                    0, half_of(source, (k, before), 1), half_of(got, (k, 1), 1), 3, 0
                ),
            )
            ring[k, 1, p] = [
                step_copy(1, q2[p].at[k, owner(p, 1, step)], got2[p].at[k, i], step, 1)
                for i, step in enumerate((2, 1, 3))
            ]
            ring[k, 2, p] = [
                step_copy(
                    2, q3[p].at[k, aligned(owner(p, 2, step) * ROWS, ROWS)], got3[p].at[k, i], step, 2
                )
                for i, step in enumerate((2, 1, 3))
            ]

    def send_to_partner(k, step):
        for p in range(3):
            a = owner(p, 0, step)
            for m, lanes, value in blocks(k, p, a, 1 - c):
                out_p = outgoing[p]
                out_p[k, a, m, :, lanes] = value.astype(BF)
            pair_copies[k, p, step].start()

    def join_partner(k, step):
        await_bytes(msg.at[0, pl.ds(0, 2)], pair_recv.at[k * 4 + STEPS.index(step)])
        for p in range(3):
            a = owner(p, 0, step)
            for m, lanes, value in blocks(k, p, a, c):
                arrived_p = pair[p]
                arrived_p[k, a, m, :, lanes] = (
                    value + arrived_p[k, a, m, :, lanes].astype(F32)
                ).astype(BF)
            if step == 2:
                ring[k, 0, p]["relay_a"].start()
                ring[k, 0, p]["relay_b"].start()
            elif step == 1:
                ring[k, 0, p]["direct_after"].start()
            elif step == 3:
                ring[k, 0, p]["direct_before"].start()

    def start_stage(k, stage):
        for i in range(3):
            for p in range(3):
                ring[k, stage, p][i].start()

    def add_into(dst, sources):
        for i in range(dst.shape[0]):
            value = sources[0][i].astype(F32)
            for source in sources[1:]:
                value += source[i].astype(F32)
            dst[i] = value.astype(dst.dtype)

    def pass_on(k):
        for p in range(3):
            source, via = pair[p], relays[p]
            await_bytes(via.at[k, 0], ring_recv.at[k * 9 + 3 + p])
            mine = half_of(source, (k, owner(p, 0, 1)), 0)
            add_into(mine, (mine, via.at[k, 0]))
            ring[k, 0, p]["summed_after"].start()
            await_bytes(via.at[k, 1], ring_recv.at[k * 9 + 6 + p])
            mine = half_of(source, (k, owner(p, 0, 3)), 1)
            add_into(mine, (mine, via.at[k, 1]))
            ring[k, 0, p]["summed_before"].start()

    def finish_first(k):
        await_bytes(feats.at[pl.ds(0, 256)], ring_recv.at[k * 9])
        for p in range(3):
            mine = pair[p].at[k, owner(p, 0, 0)]
            add_into(q2[p].at[k], (mine, got1[p].at[k, 0], got1[p].at[k, 1]))
        start_stage(k, 1)

    def finish_second(k):
        await_bytes(feats.at[pl.ds(0, 96)], ring_recv.at[k * 9 + 1])
        for p in range(3):
            value = q2[p][k, owner(p, 1, 0)].astype(F32)
            for i in range(3):
                value += got2[p][k, i].astype(F32)
            q3[p][k] = value
        start_stage(k, 2)

    def finish_third(k):
        await_bytes(feats.at[pl.ds(0, 48)], ring_recv.at[k * 9 + 2])
        start = 0
        at = pl.ds(k * ROWS, ROWS)
        for p in range(3):
            lanes = pl.ds(start, LANES[p])
            value = q3[p][k, aligned(owner(p, 2, 0) * ROWS, ROWS), :] + self_term[at, lanes]
            for i in range(3):
                value += got3[p][k, i]
            out[at, lanes] = value.astype(BF)
            start += LANES[p]

    def wait_all_sent():
        await_bytes(feats.at[pl.ds(0, 480)], sent.at[0])
        await_bytes(msg, sent.at[1])
        await_bytes(msg.at[:, pl.ds(0, 12)], sent.at[2])
        await_bytes(feats.at[pl.ds(0, 384)], sent.at[3])
        await_bytes(feats.at[pl.ds(0, 192)], sent.at[4])

    SEND = ((0, 2), (1, 2), (0, 1), (0, 3), (1, 1), (1, 3), (0, 0), (1, 0))

    make_messages(0, range(4))
    add_tiles(0, 0, SLOTS)
    for k, step in SEND:
        send_to_partner(k, step)
    make_messages(1, range(2))
    join_partner(0, 2)
    join_partner(1, 2)
    make_messages(1, range(2, 4))
    make_self_term()
    for k, step in SEND[2:]:
        join_partner(k, step)
    add_tiles(1, 0, 32)
    pass_on(0)
    pass_on(1)
    add_tiles(1, 32, SLOTS)
    for k, step in SEND:
        send_to_partner(2 + k, step)
    for k, step in SEND:
        join_partner(2 + k, step)
    pass_on(2)
    pass_on(3)
    for k in range(PIECES):
        finish_first(k)
    for k in range(PIECES):
        finish_second(k)
    for k in range(PIECES):
        finish_third(k)
    store = pltpu.make_async_copy(out, result, local.at[2])
    store.start()
    wait_all_sent()
    store.wait()


def body(node_feats, rel_weight, self_weight, bias, out_degree, adjacency, tile_index, tile_count):
    def buffers(*lead, kind=BF, rows=RING * ROWS):
        return [pltpu.VMEM((PIECES, *lead, rows, lanes), kind) for lanes in LANES]

    result = pl.pallas_call(
        kernel,
        out_shape=jax.ShapeDtypeStruct((COLS, OWN), BF),
        in_specs=[HBM, HBM, HBM, HBM, HBM, HBM, SMEM, HBM],
        out_specs=HBM,
        scratch_shapes=[
            pltpu.VMEM((1, HID), F32),
            pltpu.VMEM((REL, OWN), I32),
            pltpu.VMEM((3, 1, SLOTS), I32),
            pltpu.VMEM((COLS, OWN), BF),
            pltpu.VMEM((HID, OWN), BF),
            pltpu.VMEM((REL, HID, HID), BF),
            pltpu.VMEM((HID, HID), BF),
            pltpu.VMEM((REL, HALVES, HID // 2, HID), BF),
            pltpu.VMEM((HID, HID), BF),
            pltpu.VMEM((HID, 128), F32),
            pltpu.VMEM((COLS, OWN), F32),
            pltpu.VMEM((REL, OWN), F32),
            pltpu.VMEM((HALVES, REL * 4, HID // 2, TILE), BF),
            pltpu.VMEM((DEPTH, BATCH, TILE, TILE), I32),
            pltpu.VMEM((SLOTS, TILE, TILE), BF),
            pltpu.VMEM((SLOTS + 1, HID // 2, TILE), F32),
            pltpu.VMEM((8, 128), I32),
            pltpu.SMEM((8, 128), I32),
            *buffers(RING, RING),
            *buffers(RING, RING),
            *buffers(2, 2),
            *buffers(2, RING),
            *buffers(RING),
            *buffers(3),
            *buffers(kind=F32),
            *buffers(3, kind=F32, rows=ROWS),
            pltpu.SemaphoreType.DMA((5,)),
            pltpu.SemaphoreType.DMA((GATHER_ARRIVALS,)),
            pltpu.SemaphoreType.DMA((PAIR_ARRIVALS,)),
            pltpu.SemaphoreType.DMA((RING_ARRIVALS,)),
            pltpu.SemaphoreType.DMA((7,)),
            pltpu.SemaphoreType.DMA((DEPTH,)),
        ],
        compiler_params=pltpu.CompilerParams(
            collective_id=0, has_side_effects=True, vmem_limit_bytes=63 * 2**20
        ),
        name="relational_layer",
    )(
        node_feats.T, rel_weight, self_weight, bias.reshape(1, HID), out_degree,
        jnp.transpose(tile_index[0], (2, 0, 1)), tile_count, adjacency[0, 0],
    )
    return result.T


def solution(mesh):
    placed = (
        P("dom", "feat"),
        P(),
        P(),
        P(),
        P(None, "dom"),
        P("dom", "feat", None, None, None),
        P("dom", "feat", None, None),
        P("dom", "feat"),
    )
    return jax.shard_map(
        body, mesh=mesh, in_specs=placed, out_specs=P("dom", "feat"), check_vma=False
    )
```

```python
import jax
import jax.numpy as jnp
from jax import lax
from jax.experimental import pallas as pl
from jax.experimental.pallas import tpu as pltpu
from jax.sharding import PartitionSpec as P

MESH = pl.DeviceIdType.MESH
BF = jnp.bfloat16
F32 = jnp.float32
I32 = jnp.int32
RING = 4
HID = 512
COLS = 32
ROWS = 8
OWN = 1024
TILE = 256
SLOTS = 64
REL = 4
BLOCKS = 32
HALVES = 2
PIECES = 4
BATCH = 4
DEPTH = 8
UNROLL = 32
LANES = (384, 384, 256)
ORDER = ("xyz", "yzx", "zxy")
STEPS = (2, 1, 3, 0)
VMEM = pl.BlockSpec(memory_space=pltpu.VMEM)
SMEM = pl.BlockSpec(memory_space=pltpu.SMEM)
HBM = pl.BlockSpec(memory_space=pl.ANY)
NT = (((1,), (1,)), ((), ()))
GATHER_ARRIVALS = 2 * 3 + 1
PAIR_ARRIVALS = PIECES * 4
RING_ARRIVALS = PIECES * 5


def place():
    dom = lax.axis_index("dom")
    feat = lax.axis_index("feat")
    return dict(z=dom // 2, c=dom % 2, x=feat // RING, y=feat % RING)


def device(here, **moved):
    at = dict(here)
    for axis, step in moved.items():
        at[axis] = (at[axis] + step) % (2 if axis == "c" else RING)
    return (at["z"] * 2 + at["c"], at["x"] * RING + at["y"])


def greet(peers):
    barrier = pltpu.get_barrier_semaphore()
    for peer in peers:
        pl.semaphore_signal(barrier, inc=1, device_id=peer, device_id_type=MESH)
    pl.semaphore_wait(barrier, len(peers))


def aligned(start, size):
    return pl.ds(pl.multiple_of(start, size), size)


def sort_slots(index, live, table):
    shape = (128, 128)
    across = lax.broadcasted_iota(I32, shape, 1)
    down = lax.broadcasted_iota(I32, shape, 0)

    def row(value):
        return jnp.broadcast_to(jnp.concatenate([value, value], axis=1), shape)

    is_live = across < live
    target = jnp.where(is_live, row(index[1]), BLOCKS)
    block = row(index[0]) * 4 + row(index[2])
    key = jnp.where(across < SLOTS, target * 128 + across, 65536 + across)
    key_down = key.T
    rank = jnp.sum(jnp.where(key_down < key, 1, 0), axis=0, keepdims=True)
    rank_down = jnp.broadcast_to(rank, shape).T
    hit = rank_down == across
    target_down = target.T
    table[0:1, :] = jnp.sum(jnp.where(hit, down, 0), axis=0, keepdims=True)
    table[1:2, :] = jnp.sum(jnp.where(hit, block.T, 0), axis=0, keepdims=True)
    table[2:3, :] = jnp.sum(jnp.where(hit, target_down, 0), axis=0, keepdims=True)
    real = down < SLOTS
    upto = jnp.sum(jnp.where(real & (target_down <= across), 1, 0), axis=0, keepdims=True)
    below = jnp.sum(jnp.where(real & (target_down < across), 1, 0), axis=0, keepdims=True)
    table[3:4, :] = jnp.where(upto > below, upto, 0)


def kernel(
    nodes, rel, own, bias_hbm, degree_hbm, index_hbm, live, tiles, result,
    bias, degree, index, out,    feats, rel_in, own_in, rel_t, own_t, bias_t, self_term, inverse, msg,
    raw, cells, sums, table, order,
    out_x, out_y, out_z, pair_x, pair_y, pair_z,
    relay_x, relay_y, relay_z, got1x, got1y, got1z,
    q2x, q2y, q2z, got2x, got2y, got2z, q3x, q3y, q3z, got3x, got3y, got3z,
    sent, gather_recv, pair_recv, ring_recv, local, arrived,
):
    here = place()
    outgoing = (out_x, out_y, out_z)
    pair = (pair_x, pair_y, pair_z)
    relays = (relay_x, relay_y, relay_z)
    got1, got2, got3 = (got1x, got1y, got1z), (got2x, got2y, got2z), (got3x, got3y, got3z)
    q2, q3 = (q2x, q2y, q2z), (q3x, q3y, q3z)
    c = here["c"]

    mine = aligned((here["x"] * RING + here["y"]) * COLS, COLS)
    fetch_nodes = pltpu.make_async_copy(nodes, feats.at[mine, :], local.at[3])
    fetch_nodes.start()
    fetch_small = [
        pltpu.make_async_copy(src, dst, local.at[4 + i])
        for i, (src, dst) in enumerate(((index_hbm, index), (degree_hbm, degree), (bias_hbm, bias)))
    ]
    for fetch in fetch_small:
        fetch.start()
    fetch_rel = pltpu.make_async_copy(rel, rel_in, local.at[0])
    fetch_own = pltpu.make_async_copy(own, own_in, local.at[1])
    fetch_rel.start()
    fetch_own.start()

    def fetch_tiles(batch, slot):
        return pltpu.make_async_copy(
            tiles.at[pl.ds(batch * BATCH, BATCH)], raw.at[slot], arrived.at[slot]
        )

    for batch in range(DEPTH):
        fetch_tiles(batch, batch).start()
    partner = device(here, c=1)
    peers = [device(here, **{axis: step}) for axis in "xy" for step in (1, 2, 3)]
    peers += [device(here, z=step) for step in (1, 3)] + [partner]
    greet(peers)

    half = COLS // 2
    first_axis = ("x", "y")
    second_axis = ("y", "x")

    def rows(h, x, y):
        return aligned((x * RING + y) * COLS + h * half, half)


    def remote(src, dst, peer, arrival):
        return pltpu.make_async_remote_copy(
            src_ref=src, dst_ref=dst, send_sem=sent.at[0], recv_sem=gather_recv.at[arrival],
            device_id=peer, device_id_type=MESH,
        )

    def part(h, a):
        at = dict(here)
        at[first_axis[h]] = (at[first_axis[h]] + a) % RING
        return feats.at[rows(h, at["x"], at["y"]), :]

    fetch_nodes.wait()
    for step in (1, 3, 2):
        for h in (0, 1):
            peer = device(here, **{first_axis[h]: step})
            remote(part(h, 0), part(h, 0), peer, h * 3 + RING - step - 1).start()

    def spread(h, a):
        for step in (2, 1, 3):
            peer = device(here, **{second_axis[h]: step})
            remote(part(h, a), part(h, a), peer, GATHER_ARRIVALS - 1).start()

    for h in (0, 1):
        spread(h, 0)

    def forward(i):
        for h in (0, 1):
            at = here[first_axis[h]]
            other = i + jnp.where(at <= i, 1, 0)
            a = (other - at + RING) % RING
            piece = part(h, a)
            pltpu.make_async_copy(piece, piece, gather_recv.at[h * 3 + a - 1]).wait()
            spread(h, a)

    def transpose(r):
        turned = rel_in[r].astype(F32).T.reshape(HID // COLS, HALVES, 2, ROWS, HID)
        for h in range(HALVES):
            for i in range(2):
                some = turned[:, h, i].reshape(HID // PIECES, HID)
                rel_t[r, h, pl.ds(i * (HID // PIECES), HID // PIECES), :] = some.astype(BF)

    def convert(low, high):
        def one(batch, carry):
            slot = batch % DEPTH
            fetch_tiles(batch, slot).wait()

            def tile(i, carry):
                cells[batch * BATCH + i] = raw[slot, i].astype(F32).astype(BF)
                return carry

            lax.fori_loop(0, BATCH, tile, 0, unroll=2)

            @pl.when(batch + DEPTH < SLOTS // BATCH)
            def _():
                fetch_tiles(batch + DEPTH, slot).start()

            return carry

        lax.fori_loop(low, high, one, 0)

    for fetch in fetch_small:
        fetch.wait()
    inverse[...] = 1.0 / jnp.maximum(degree[...], 1).astype(F32)
    sort_slots(index, live[0, 0], table)
    fetch_order = pltpu.make_async_copy(table, order, local.at[2])
    fetch_order.start()
    sums[0] = jnp.zeros((HID // 2, TILE), F32)
    fetch_rel.wait()
    fetch_own.wait()
    for r in range(REL):
        transpose(r)
    convert(0, 6)
    forward(0)
    forward(1)
    forward(2)
    own_t[...] = own_in[...].T
    bias_t[...] = jnp.broadcast_to(bias[...], (128, HID)).T
    convert(6, SLOTS // BATCH)
    fetch_order.wait()
    rest = feats.at[pl.ds(0, 384)]
    pltpu.make_async_copy(rest, rest, gather_recv.at[GATHER_ARRIVALS - 1]).wait()

    def make_messages(h, sources):
        for s in sources:
            at = pl.ds(s * TILE, TILE)

            def relation(r, carry):
                product = jnp.dot(rel_t[r, h], feats[:, at], preferred_element_type=F32)
                msg[h, r * 4 + s] = (product * inverse[pl.ds(r, 1), at]).astype(BF)
                return carry

            lax.fori_loop(0, REL, relation, 0, unroll=True)

    def make_self_term():
        bias_rows = bias_t[mine, :]
        for s in range(OWN // TILE):
            at = pl.ds(s * TILE, TILE)
            self_term[:, at] = jnp.dot(
                own_t[mine, :], feats[:, at], preferred_element_type=F32
            ) + jnp.concatenate([bias_rows, bias_rows], axis=1)

    def add_tiles(h, low, high, unroll=UNROLL):
        def some(i, carry):
            for u in range(unroll):
                t = i * unroll + u
                product = lax.dot_general(
                    msg[h, order[1, t]], cells[order[0, t]], NT, preferred_element_type=F32
                )
                before = order[2, jnp.maximum(t - 1, 0)]
                same = jnp.where((t > 0) & (order[2, t] == before), 1.0, 0.0)
                sums[t + 1] = sums[t] * same + product
            return carry

        lax.fori_loop(low // unroll, high // unroll, some, 0)

    def owner(p, stage, step):
        return (here[ORDER[p][stage]] + step) % RING

    def blocks(k, p, a, core):
        start = k % 2 * (HID // PIECES)

        def at(x, y):
            return aligned(start + (x * RING + y) * ROWS, ROWS)

        def last(z, b):
            return order[3, z * 8 + core * 4 + b]

        if p == 2:
            for x in range(RING):
                rows = aligned(start + x * RING * ROWS, RING * ROWS)
                yield x, pl.ds(0, 256), sums[last(a, 3), rows, :]
            return
        for m in range(RING):
            if p == 0:
                one = [sums[last(z, 0), at(a, m), :] for z in range(RING)]
                two = [sums[last(z, 1), at(a, m), 0:128] for z in range(RING)]
            else:
                one = [sums[last(m, 1), at(x, a), 128:256] for x in range(RING)]
                two = [sums[last(m, 2), at(x, a), :] for x in range(RING)]
            width = one[0].shape[1]
            yield m, pl.ds(0, width), jnp.concatenate(one, axis=0)
            yield m, pl.ds(width, 384 - width), jnp.concatenate(two, axis=0)

    def await_bytes(ref, semaphore):
        pltpu.make_async_copy(ref, ref, semaphore).wait()

    pair_copies = {}
    for k in range(PIECES):
        for n, step in enumerate(STEPS):
            for p in range(3):
                a = owner(p, 0, step)
                pair_copies[k, p, step] = pltpu.make_async_remote_copy(
                    src_ref=outgoing[p].at[k, a], dst_ref=pair[p].at[k, a],
                    send_sem=sent.at[1], recv_sem=pair_recv.at[k * 4 + n],
                    device_id=partner, device_id_type=MESH,
                )

    def half_of(ref, lead, which):
        n = ref.shape[len(lead)] // 2
        return ref.at[(*lead, pl.ds(which * n, n))]

    ring = {}
    for k in range(PIECES):
        for p in range(3):

            def step_copy(stage, src, dst, step, arrival):
                return pltpu.make_async_remote_copy(
                    src_ref=src, dst_ref=dst, send_sem=sent.at[2 + stage],
                    recv_sem=ring_recv.at[k * 5 + arrival],
                    device_id=device(here, **{ORDER[p][stage]: step}), device_id_type=MESH,
                )

            opposite, after, before = (owner(p, 0, step) for step in (2, 1, 3))
            source, via, got = pair[p], relays[p], got1[p]
            ring[k, 0, p] = dict(
                relay_a=step_copy(0, half_of(source, (k, opposite), 0), via.at[k, 0], 1, 3),
                relay_b=step_copy(0, half_of(source, (k, opposite), 1), via.at[k, 1], 3, 4),
                direct_after=step_copy(
                    0, half_of(source, (k, after), 1), half_of(got, (k, 0), 1), 1, 0
                ),
                direct_before=step_copy(
                    0, half_of(source, (k, before), 0), half_of(got, (k, 1), 0), 3, 0
                ),
                summed_after=step_copy(
                    0, half_of(source, (k, after), 0), half_of(got, (k, 0), 0), 1, 0
                ),
                summed_before=step_copy(
                    0, half_of(source, (k, before), 1), half_of(got, (k, 1), 1), 3, 0
                ),
            )
            ring[k, 1, p] = [
                step_copy(1, q2[p].at[k, owner(p, 1, step)], got2[p].at[k, i], step, 1)
                for i, step in enumerate((2, 1, 3))
            ]
            ring[k, 2, p] = [
                step_copy(
                    2, q3[p].at[k, aligned(owner(p, 2, step) * ROWS, ROWS)], got3[p].at[k, i], step, 2
                )
                for i, step in enumerate((2, 1, 3))
            ]

    def send_to_partner(k, step):
        for p in range(3):
            a = owner(p, 0, step)
            for m, lanes, value in blocks(k, p, a, 1 - c):
                out_p = outgoing[p]
                out_p[k, a, m, :, lanes] = value.astype(BF)
            pair_copies[k, p, step].start()

    def join_partner(k, step):
        await_bytes(msg.at[0, pl.ds(0, 2)], pair_recv.at[k * 4 + STEPS.index(step)])
        for p in range(3):
            a = owner(p, 0, step)
            for m, lanes, value in blocks(k, p, a, c):
                arrived_p = pair[p]
                arrived_p[k, a, m, :, lanes] = (
                    value + arrived_p[k, a, m, :, lanes].astype(F32)
                ).astype(BF)
            if step == 2:
                ring[k, 0, p]["relay_a"].start()
                ring[k, 0, p]["relay_b"].start()
            elif step == 1:
                ring[k, 0, p]["direct_after"].start()
            elif step == 3:
                ring[k, 0, p]["direct_before"].start()

    def start_stage(k, stage):
        for i in range(3):
            for p in range(3):
                ring[k, stage, p][i].start()

    def add_into(dst, sources):
        for i in range(dst.shape[0]):
            value = sources[0][i].astype(F32)
            for source in sources[1:]:
                value += source[i].astype(F32)
            dst[i] = value.astype(dst.dtype)

    def pass_on(k):
        for way, step, name in ((0, 1, "summed_after"), (1, 3, "summed_before")):
            await_bytes(feats.at[pl.ds(0, 64)], ring_recv.at[k * 5 + 3 + way])
            for p in range(3):
                mine = half_of(pair[p], (k, owner(p, 0, step)), way)
                add_into(mine, (mine, relays[p].at[k, way]))
                ring[k, 0, p][name].start()

    def finish_first(k):
        await_bytes(feats.at[pl.ds(0, 256)], ring_recv.at[k * 5])
        for p in range(3):
            mine = pair[p].at[k, owner(p, 0, 0)]
            add_into(q2[p].at[k], (mine, got1[p].at[k, 0], got1[p].at[k, 1]))
        start_stage(k, 1)

    def finish_second(k):
        await_bytes(feats.at[pl.ds(0, 96)], ring_recv.at[k * 5 + 1])
        for p in range(3):
            value = q2[p][k, owner(p, 1, 0)].astype(F32)
            for i in range(3):
                value += got2[p][k, i].astype(F32)
            q3[p][k] = value
        start_stage(k, 2)

    def finish_third(k):
        await_bytes(feats.at[pl.ds(0, 48)], ring_recv.at[k * 5 + 2])
        start = 0
        at = pl.ds(k * ROWS, ROWS)
        for p in range(3):
            lanes = pl.ds(start, LANES[p])
            value = q3[p][k, aligned(owner(p, 2, 0) * ROWS, ROWS), :] + self_term[at, lanes]
            for i in range(3):
                value += got3[p][k, i]
            out[at, lanes] = value.astype(BF)
            start += LANES[p]

    def wait_all_sent():
        await_bytes(feats.at[pl.ds(0, 480)], sent.at[0])
        await_bytes(msg, sent.at[1])
        await_bytes(msg.at[:, pl.ds(0, 12)], sent.at[2])
        await_bytes(feats.at[pl.ds(0, 384)], sent.at[3])
        await_bytes(feats.at[pl.ds(0, 192)], sent.at[4])

    SEND = ((0, 2), (1, 2), (0, 1), (0, 3), (1, 1), (1, 3), (0, 0), (1, 0))

    make_messages(0, range(4))
    add_tiles(0, 0, SLOTS)
    for k, step in SEND:
        send_to_partner(k, step)
    make_messages(1, range(2))
    join_partner(0, 2)
    join_partner(1, 2)
    make_messages(1, range(2, 4))
    for k, step in SEND[2:]:
        join_partner(k, step)
    add_tiles(1, 0, 48, 24)
    pass_on(0)
    add_tiles(1, 48, SLOTS, 16)
    for k, step in SEND[:2]:
        send_to_partner(2 + k, step)
    pass_on(1)
    for k, step in SEND[2:]:
        send_to_partner(2 + k, step)
    for k, step in SEND:
        join_partner(2 + k, step)
    make_self_term()
    pass_on(2)
    pass_on(3)
    for k in range(PIECES):
        finish_first(k)
    for k in range(PIECES):
        finish_second(k)
    for k in range(PIECES):
        finish_third(k)
    store = pltpu.make_async_copy(out, result, local.at[2])
    store.start()
    wait_all_sent()
    store.wait()


def body(node_feats, rel_weight, self_weight, bias, out_degree, adjacency, tile_index, tile_count):
    def buffers(*lead, kind=BF, rows=RING * ROWS):
        return [pltpu.VMEM((PIECES, *lead, rows, lanes), kind) for lanes in LANES]

    result = pl.pallas_call(
        kernel,
        out_shape=jax.ShapeDtypeStruct((COLS, OWN), BF),
        in_specs=[HBM, HBM, HBM, HBM, HBM, HBM, SMEM, HBM],
        out_specs=HBM,
        scratch_shapes=[
            pltpu.VMEM((1, HID), F32),
            pltpu.VMEM((REL, OWN), I32),
            pltpu.VMEM((3, 1, SLOTS), I32),
            pltpu.VMEM((COLS, OWN), BF),
            pltpu.VMEM((HID, OWN), BF),
            pltpu.VMEM((REL, HID, HID), BF),
            pltpu.VMEM((HID, HID), BF),
            pltpu.VMEM((REL, HALVES, HID // 2, HID), BF),
            pltpu.VMEM((HID, HID), BF),
            pltpu.VMEM((HID, 128), F32),
            pltpu.VMEM((COLS, OWN), F32),
            pltpu.VMEM((REL, OWN), F32),
            pltpu.VMEM((HALVES, REL * 4, HID // 2, TILE), BF),
            pltpu.VMEM((DEPTH, BATCH, TILE, TILE), I32),
            pltpu.VMEM((SLOTS, TILE, TILE), BF),
            pltpu.VMEM((SLOTS + 1, HID // 2, TILE), F32),
            pltpu.VMEM((8, 128), I32),
            pltpu.SMEM((8, 128), I32),
            *buffers(RING, RING),
            *buffers(RING, RING),
            *buffers(2, 2),
            *buffers(2, RING),
            *buffers(RING),
            *buffers(3),
            *buffers(kind=F32),
            *buffers(3, kind=F32, rows=ROWS),
            pltpu.SemaphoreType.DMA((5,)),
            pltpu.SemaphoreType.DMA((GATHER_ARRIVALS,)),
            pltpu.SemaphoreType.DMA((PAIR_ARRIVALS,)),
            pltpu.SemaphoreType.DMA((RING_ARRIVALS,)),
            pltpu.SemaphoreType.DMA((7,)),
            pltpu.SemaphoreType.DMA((DEPTH,)),
        ],
        compiler_params=pltpu.CompilerParams(
            collective_id=0, has_side_effects=True, vmem_limit_bytes=63 * 2**20
        ),
        name="relational_layer",
    )(
        node_feats.T, rel_weight, self_weight, bias.reshape(1, HID), out_degree,
        jnp.transpose(tile_index[0], (2, 0, 1)), tile_count, adjacency[0, 0],
    )
    return result.T


def solution(mesh):
    placed = (
        P("dom", "feat"),
        P(),
        P(),
        P(),
        P(None, "dom"),
        P("dom", "feat", None, None, None),
        P("dom", "feat", None, None),
        P("dom", "feat"),
    )
    return jax.shard_map(
        body, mesh=mesh, in_specs=placed, out_specs=P("dom", "feat"), check_vma=False
    )
```

```python
import jax
import jax.numpy as jnp
from jax import lax
from jax.experimental import pallas as pl
from jax.experimental.pallas import tpu as pltpu
from jax.sharding import PartitionSpec as P

MESH = pl.DeviceIdType.MESH
BF = jnp.bfloat16
F32 = jnp.float32
I32 = jnp.int32
RING = 4
HID = 512
COLS = 32
ROWS = 8
OWN = 1024
TILE = 256
SLOTS = 64
REL = 4
BLOCKS = 32
HALVES = 2
PIECES = 4
BATCH = 4
DEPTH = 8
UNROLL = 32
LANES = (384, 384, 256)
ORDER = ("xyz", "yzx", "zxy")
STEPS = (2, 1, 3, 0)
VMEM = pl.BlockSpec(memory_space=pltpu.VMEM)
SMEM = pl.BlockSpec(memory_space=pltpu.SMEM)
HBM = pl.BlockSpec(memory_space=pl.ANY)
NT = (((1,), (1,)), ((), ()))
GATHER_ARRIVALS = 2 * 3 + 1
PAIR_ARRIVALS = PIECES * 6
RING_ARRIVALS = PIECES * 5


def place():
    dom = lax.axis_index("dom")
    feat = lax.axis_index("feat")
    return dict(z=dom // 2, c=dom % 2, x=feat // RING, y=feat % RING)


def device(here, **moved):
    at = dict(here)
    for axis, step in moved.items():
        at[axis] = (at[axis] + step) % (2 if axis == "c" else RING)
    return (at["z"] * 2 + at["c"], at["x"] * RING + at["y"])


def greet(peers):
    barrier = pltpu.get_barrier_semaphore()
    for peer in peers:
        pl.semaphore_signal(barrier, inc=1, device_id=peer, device_id_type=MESH)
    pl.semaphore_wait(barrier, len(peers))


def aligned(start, size):
    return pl.ds(pl.multiple_of(start, size), size)


def sort_slots(index, live, table):
    shape = (128, 128)
    across = lax.broadcasted_iota(I32, shape, 1)
    down = lax.broadcasted_iota(I32, shape, 0)

    def row(value):
        return jnp.broadcast_to(jnp.concatenate([value, value], axis=1), shape)

    is_live = across < live
    target = jnp.where(is_live, row(index[1]), BLOCKS)
    block = row(index[0]) * 4 + row(index[2])
    key = jnp.where(across < SLOTS, target * 128 + across, 65536 + across)
    key_down = key.T
    rank = jnp.sum(jnp.where(key_down < key, 1, 0), axis=0, keepdims=True)
    rank_down = jnp.broadcast_to(rank, shape).T
    hit = rank_down == across
    target_down = target.T
    table[0:1, :] = jnp.sum(jnp.where(hit, down, 0), axis=0, keepdims=True)
    table[1:2, :] = jnp.sum(jnp.where(hit, block.T, 0), axis=0, keepdims=True)
    table[2:3, :] = jnp.sum(jnp.where(hit, target_down, 0), axis=0, keepdims=True)
    real = down < SLOTS
    upto = jnp.sum(jnp.where(real & (target_down <= across), 1, 0), axis=0, keepdims=True)
    below = jnp.sum(jnp.where(real & (target_down < across), 1, 0), axis=0, keepdims=True)
    table[3:4, :] = jnp.where(upto > below, upto, 0)


def kernel(
    nodes, rel, own, bias_hbm, degree_hbm, index_hbm, live, tiles, result,
    bias, degree, index, out,    feats, rel_in, own_in, rel_t, own_t, bias_t, self_term, inverse, msg,
    raw, cells, sums, table, order,
    out_x, out_y, out_z, pair_x, pair_y, pair_z,
    relay_x, relay_y, relay_z, got1x, got1y, got1z,
    q2x, q2y, q2z, got2x, got2y, got2z, q3x, q3y, q3z, got3x, got3y, got3z,
    sent, gather_recv, pair_recv, ring_recv, local, arrived,
):
    here = place()
    outgoing = (out_x, out_y, out_z)
    pair = (pair_x, pair_y, pair_z)
    relays = (relay_x, relay_y, relay_z)
    got1, got2, got3 = (got1x, got1y, got1z), (got2x, got2y, got2z), (got3x, got3y, got3z)
    q2, q3 = (q2x, q2y, q2z), (q3x, q3y, q3z)
    c = here["c"]

    mine = aligned((here["x"] * RING + here["y"]) * COLS, COLS)
    fetch_nodes = pltpu.make_async_copy(nodes, feats.at[mine, :], local.at[3])
    fetch_nodes.start()
    fetch_small = [
        pltpu.make_async_copy(src, dst, local.at[4 + i])
        for i, (src, dst) in enumerate(((index_hbm, index), (degree_hbm, degree), (bias_hbm, bias)))
    ]
    for fetch in fetch_small:
        fetch.start()
    fetch_rel = pltpu.make_async_copy(rel, rel_in, local.at[0])
    fetch_own = pltpu.make_async_copy(own, own_in, local.at[1])
    fetch_rel.start()
    fetch_own.start()

    def fetch_tiles(batch, slot):
        return pltpu.make_async_copy(
            tiles.at[pl.ds(batch * BATCH, BATCH)], raw.at[slot], arrived.at[slot]
        )

    for batch in range(DEPTH):
        fetch_tiles(batch, batch).start()
    partner = device(here, c=1)
    peers = [device(here, **{axis: step}) for axis in "xy" for step in (1, 2, 3)]
    peers += [device(here, z=step) for step in (1, 3)] + [partner]
    greet(peers)

    half = COLS // 2
    first_axis = ("x", "y")
    second_axis = ("y", "x")

    def rows(h, x, y):
        return aligned((x * RING + y) * COLS + h * half, half)


    def remote(src, dst, peer, arrival):
        return pltpu.make_async_remote_copy(
            src_ref=src, dst_ref=dst, send_sem=sent.at[0], recv_sem=gather_recv.at[arrival],
            device_id=peer, device_id_type=MESH,
        )

    def part(h, a):
        at = dict(here)
        at[first_axis[h]] = (at[first_axis[h]] + a) % RING
        return feats.at[rows(h, at["x"], at["y"]), :]

    fetch_nodes.wait()
    for step in (1, 3, 2):
        for h in (0, 1):
            peer = device(here, **{first_axis[h]: step})
            remote(part(h, 0), part(h, 0), peer, h * 3 + RING - step - 1).start()

    def spread(h, a):
        for step in (2, 1, 3):
            peer = device(here, **{second_axis[h]: step})
            remote(part(h, a), part(h, a), peer, GATHER_ARRIVALS - 1).start()

    for h in (0, 1):
        spread(h, 0)

    def forward(i):
        for h in (0, 1):
            at = here[first_axis[h]]
            other = i + jnp.where(at <= i, 1, 0)
            a = (other - at + RING) % RING
            piece = part(h, a)
            pltpu.make_async_copy(piece, piece, gather_recv.at[h * 3 + a - 1]).wait()
            spread(h, a)

    def transpose(r):
        turned = rel_in[r].astype(F32).T.reshape(HID // COLS, HALVES, 2, ROWS, HID)
        for h in range(HALVES):
            for i in range(2):
                some = turned[:, h, i].reshape(HID // PIECES, HID)
                rel_t[r, h, pl.ds(i * (HID // PIECES), HID // PIECES), :] = some.astype(BF)

    def convert(low, high):
        def one(batch, carry):
            slot = batch % DEPTH
            fetch_tiles(batch, slot).wait()

            def tile(i, carry):
                cells[batch * BATCH + i] = raw[slot, i].astype(F32).astype(BF)
                return carry

            lax.fori_loop(0, BATCH, tile, 0, unroll=2)

            @pl.when(batch + DEPTH < SLOTS // BATCH)
            def _():
                fetch_tiles(batch + DEPTH, slot).start()

            return carry

        lax.fori_loop(low, high, one, 0)

    for fetch in fetch_small:
        fetch.wait()
    inverse[...] = 1.0 / jnp.maximum(degree[...], 1).astype(F32)
    sort_slots(index, live[0, 0], table)
    fetch_order = pltpu.make_async_copy(table, order, local.at[2])
    fetch_order.start()
    sums[0] = jnp.zeros((HID // 2, TILE), F32)
    fetch_rel.wait()
    fetch_own.wait()
    for r in range(REL):
        transpose(r)
    convert(0, 6)
    forward(0)
    forward(1)
    forward(2)
    own_t[...] = own_in[...].T
    bias_t[...] = jnp.broadcast_to(bias[...], (128, HID)).T
    convert(6, SLOTS // BATCH)
    fetch_order.wait()
    rest = feats.at[pl.ds(0, 384)]
    pltpu.make_async_copy(rest, rest, gather_recv.at[GATHER_ARRIVALS - 1]).wait()

    def make_messages(h, sources):
        for s in sources:
            at = pl.ds(s * TILE, TILE)

            def relation(r, carry):
                product = jnp.dot(rel_t[r, h], feats[:, at], preferred_element_type=F32)
                msg[h, r * 4 + s] = (product * inverse[pl.ds(r, 1), at]).astype(BF)
                return carry

            lax.fori_loop(0, REL, relation, 0, unroll=True)

    def make_self_term():
        bias_rows = bias_t[mine, :]
        for s in range(OWN // TILE):
            at = pl.ds(s * TILE, TILE)
            self_term[:, at] = jnp.dot(
                own_t[mine, :], feats[:, at], preferred_element_type=F32
            ) + jnp.concatenate([bias_rows, bias_rows], axis=1)

    def add_tiles(h, low, high, unroll=UNROLL):
        def some(i, carry):
            for u in range(unroll):
                t = i * unroll + u
                product = lax.dot_general(
                    msg[h, order[1, t]], cells[order[0, t]], NT, preferred_element_type=F32
                )
                before = order[2, jnp.maximum(t - 1, 0)]
                same = jnp.where((t > 0) & (order[2, t] == before), 1.0, 0.0)
                sums[t + 1] = sums[t] * same + product
            return carry

        lax.fori_loop(low // unroll, high // unroll, some, 0)

    def owner(p, stage, step):
        return (here[ORDER[p][stage]] + step) % RING

    def blocks(k, p, a, core):
        start = k % 2 * (HID // PIECES)

        def at(x, y):
            return aligned(start + (x * RING + y) * ROWS, ROWS)

        def last(z, b):
            return order[3, z * 8 + core * 4 + b]

        if p == 2:
            for x in range(RING):
                rows = aligned(start + x * RING * ROWS, RING * ROWS)
                yield x, pl.ds(0, 256), sums[last(a, 3), rows, :]
            return
        if p == 0:
            rows = aligned(start + a * RING * ROWS, RING * ROWS)
            for b, lanes in ((0, pl.ds(0, 256)), (1, pl.ds(0, 128))):
                found = [sums[last(z, b), rows, lanes] for z in range(RING)]
                for m in range(RING):
                    some = [value[m * ROWS : (m + 1) * ROWS] for value in found]
                    yield m, pl.ds(256 * b, lanes.size), jnp.concatenate(some, axis=0)
            return
        places = [at(x, a) for x in range(RING)]
        for b, lanes, to in ((1, pl.ds(128, 128), 0), (2, pl.ds(0, 256), 128)):
            for m in range(RING):
                end = last(m, b)
                some = [sums[end, place_x, lanes] for place_x in places]
                yield m, pl.ds(to, lanes.size), jnp.concatenate(some, axis=0)

    def await_bytes(ref, semaphore):
        pltpu.make_async_copy(ref, ref, semaphore).wait()

    pair_copies = {}
    for k in range(PIECES):
        for n, step in enumerate(STEPS):
            for p in range(3):
                a = owner(p, 0, step)
                pair_copies[k, p, step] = pltpu.make_async_remote_copy(
                    src_ref=outgoing[p].at[k, a], dst_ref=pair[p].at[k, a],
                    send_sem=sent.at[1], recv_sem=pair_recv.at[k * 6 + (p if step == 2 else 2 + n)],
                    device_id=partner, device_id_type=MESH,
                )

    def half_of(ref, lead, which):
        n = ref.shape[len(lead)] // 2
        return ref.at[(*lead, pl.ds(which * n, n))]

    ring = {}
    for k in range(PIECES):
        for p in range(3):

            def step_copy(stage, src, dst, step, arrival):
                return pltpu.make_async_remote_copy(
                    src_ref=src, dst_ref=dst, send_sem=sent.at[2 + stage],
                    recv_sem=ring_recv.at[k * 5 + arrival],
                    device_id=device(here, **{ORDER[p][stage]: step}), device_id_type=MESH,
                )

            opposite, after, before = (owner(p, 0, step) for step in (2, 1, 3))
            source, via, got = pair[p], relays[p], got1[p]
            ring[k, 0, p] = dict(
                relay_a=step_copy(0, half_of(source, (k, opposite), 0), via.at[k, 0], 1, 3),
                relay_b=step_copy(0, half_of(source, (k, opposite), 1), via.at[k, 1], 3, 4),
                direct_after=step_copy(
                    0, half_of(source, (k, after), 1), half_of(got, (k, 0), 1), 1, 0
                ),
                direct_before=step_copy(
                    0, half_of(source, (k, before), 0), half_of(got, (k, 1), 0), 3, 0
                ),
                summed_after=step_copy(
                    0, half_of(source, (k, after), 0), half_of(got, (k, 0), 0), 1, 0
                ),
                summed_before=step_copy(
                    0, half_of(source, (k, before), 1), half_of(got, (k, 1), 1), 3, 0
                ),
            )
            ring[k, 1, p] = [
                step_copy(1, q2[p].at[k, owner(p, 1, step)], got2[p].at[k, i], step, 1)
                for i, step in enumerate((2, 1, 3))
            ]
            ring[k, 2, p] = [
                step_copy(
                    2, q3[p].at[k, aligned(owner(p, 2, step) * ROWS, ROWS)], got3[p].at[k, i], step, 2
                )
                for i, step in enumerate((2, 1, 3))
            ]

    def send_to_partner(k, step):
        for p in range(3):
            a = owner(p, 0, step)
            for m, lanes, value in blocks(k, p, a, 1 - c):
                out_p = outgoing[p]
                out_p[k, a, m, :, lanes] = value.astype(BF)
            pair_copies[k, p, step].start()

    def join_partner(k, step):
        if step != 2:
            await_bytes(msg.at[0, pl.ds(0, 2)], pair_recv.at[k * 6 + 2 + STEPS.index(step)])
        for p in range(3):
            a = owner(p, 0, step)
            if step == 2:
                await_bytes(pair[p].at[k, a], pair_recv.at[k * 6 + p])
            for m, lanes, value in blocks(k, p, a, c):
                arrived_p = pair[p]
                arrived_p[k, a, m, :, lanes] = (
                    value + arrived_p[k, a, m, :, lanes].astype(F32)
                ).astype(BF)
            if step == 2:
                ring[k, 0, p]["relay_a"].start()
                ring[k, 0, p]["relay_b"].start()
            elif step == 1:
                ring[k, 0, p]["direct_after"].start()
            elif step == 3:
                ring[k, 0, p]["direct_before"].start()

    def start_stage(k, stage):
        for i in range(3):
            for p in range(3):
                ring[k, stage, p][i].start()

    def add_into(dst, sources):
        for i in range(dst.shape[0]):
            value = sources[0][i].astype(F32)
            for source in sources[1:]:
                value += source[i].astype(F32)
            dst[i] = value.astype(dst.dtype)

    def pass_on(k):
        for way, step, name in ((0, 1, "summed_after"), (1, 3, "summed_before")):
            await_bytes(feats.at[pl.ds(0, 64)], ring_recv.at[k * 5 + 3 + way])
            for p in range(3):
                mine = half_of(pair[p], (k, owner(p, 0, step)), way)
                add_into(mine, (mine, relays[p].at[k, way]))
                ring[k, 0, p][name].start()

    def finish_first(k):
        await_bytes(feats.at[pl.ds(0, 256)], ring_recv.at[k * 5])
        for p in range(3):
            mine = pair[p].at[k, owner(p, 0, 0)]
            add_into(q2[p].at[k], (mine, got1[p].at[k, 0], got1[p].at[k, 1]))
        start_stage(k, 1)

    def finish_second(k):
        await_bytes(feats.at[pl.ds(0, 96)], ring_recv.at[k * 5 + 1])
        for p in range(3):
            value = q2[p][k, owner(p, 1, 0)].astype(F32)
            for i in range(3):
                value += got2[p][k, i].astype(F32)
            q3[p][k] = value
        start_stage(k, 2)

    def finish_third(k):
        await_bytes(feats.at[pl.ds(0, 48)], ring_recv.at[k * 5 + 2])
        start = 0
        at = pl.ds(k * ROWS, ROWS)
        for p in range(3):
            lanes = pl.ds(start, LANES[p])
            value = q3[p][k, aligned(owner(p, 2, 0) * ROWS, ROWS), :] + self_term[at, lanes]
            for i in range(3):
                value += got3[p][k, i]
            out[at, lanes] = value.astype(BF)
            start += LANES[p]

    def wait_all_sent():
        await_bytes(feats.at[pl.ds(0, 480)], sent.at[0])
        await_bytes(msg, sent.at[1])
        await_bytes(msg.at[:, pl.ds(0, 12)], sent.at[2])
        await_bytes(feats.at[pl.ds(0, 384)], sent.at[3])
        await_bytes(feats.at[pl.ds(0, 192)], sent.at[4])

    SEND = ((0, 2), (1, 2), (0, 1), (0, 3), (1, 1), (1, 3), (0, 0), (1, 0))

    make_messages(0, range(4))
    add_tiles(0, 0, SLOTS)
    for k, step in SEND:
        send_to_partner(k, step)
    make_messages(1, range(2))
    join_partner(0, 2)
    join_partner(1, 2)
    make_messages(1, range(2, 4))
    for k, step in SEND[2:]:
        join_partner(k, step)
    add_tiles(1, 0, 48, 24)
    pass_on(0)
    add_tiles(1, 48, SLOTS, 16)
    for k, step in SEND[:2]:
        send_to_partner(2 + k, step)
    pass_on(1)
    for k, step in SEND[2:]:
        send_to_partner(2 + k, step)
    for k, step in SEND:
        join_partner(2 + k, step)
    make_self_term()
    pass_on(2)
    pass_on(3)
    for k in range(PIECES):
        finish_first(k)
    for k in range(PIECES):
        finish_second(k)
    for k in range(PIECES):
        finish_third(k)
    store = pltpu.make_async_copy(out, result, local.at[2])
    store.start()
    wait_all_sent()
    store.wait()


def body(node_feats, rel_weight, self_weight, bias, out_degree, adjacency, tile_index, tile_count):
    def buffers(*lead, kind=BF, rows=RING * ROWS):
        return [pltpu.VMEM((PIECES, *lead, rows, lanes), kind) for lanes in LANES]

    result = pl.pallas_call(
        kernel,
        out_shape=jax.ShapeDtypeStruct((COLS, OWN), BF),
        in_specs=[HBM, HBM, HBM, HBM, HBM, HBM, SMEM, HBM],
        out_specs=HBM,
        scratch_shapes=[
            pltpu.VMEM((1, HID), F32),
            pltpu.VMEM((REL, OWN), I32),
            pltpu.VMEM((3, 1, SLOTS), I32),
            pltpu.VMEM((COLS, OWN), BF),
            pltpu.VMEM((HID, OWN), BF),
            pltpu.VMEM((REL, HID, HID), BF),
            pltpu.VMEM((HID, HID), BF),
            pltpu.VMEM((REL, HALVES, HID // 2, HID), BF),
            pltpu.VMEM((HID, HID), BF),
            pltpu.VMEM((HID, 128), F32),
            pltpu.VMEM((COLS, OWN), F32),
            pltpu.VMEM((REL, OWN), F32),
            pltpu.VMEM((HALVES, REL * 4, HID // 2, TILE), BF),
            pltpu.VMEM((DEPTH, BATCH, TILE, TILE), I32),
            pltpu.VMEM((SLOTS, TILE, TILE), BF),
            pltpu.VMEM((SLOTS + 1, HID // 2, TILE), F32),
            pltpu.VMEM((8, 128), I32),
            pltpu.SMEM((8, 128), I32),
            *buffers(RING, RING),
            *buffers(RING, RING),
            *buffers(2, 2),
            *buffers(2, RING),
            *buffers(RING),
            *buffers(3),
            *buffers(kind=F32),
            *buffers(3, kind=F32, rows=ROWS),
            pltpu.SemaphoreType.DMA((5,)),
            pltpu.SemaphoreType.DMA((GATHER_ARRIVALS,)),
            pltpu.SemaphoreType.DMA((PAIR_ARRIVALS,)),
            pltpu.SemaphoreType.DMA((RING_ARRIVALS,)),
            pltpu.SemaphoreType.DMA((7,)),
            pltpu.SemaphoreType.DMA((DEPTH,)),
        ],
        compiler_params=pltpu.CompilerParams(
            collective_id=0, has_side_effects=True, vmem_limit_bytes=63 * 2**20
        ),
        name="relational_layer",
    )(
        node_feats.T, rel_weight, self_weight, bias.reshape(1, HID), out_degree,
        jnp.transpose(tile_index[0], (2, 0, 1)), tile_count, adjacency[0, 0],
    )
    return result.T


def solution(mesh):
    placed = (
        P("dom", "feat"),
        P(),
        P(),
        P(),
        P(None, "dom"),
        P("dom", "feat", None, None, None),
        P("dom", "feat", None, None),
        P("dom", "feat"),
    )
    return jax.shard_map(
        body, mesh=mesh, in_specs=placed, out_specs=P("dom", "feat"), check_vma=False
    )
```
